64 devices in a mesh: dp: 4 (over x, y), tp: 16 (over z, core).
Axes of the slice: x: 2, y: 2, z: 8, core: 2. Of those that a mesh axis runs over, the one named last changes fastest.
The devices are a block of a 4x4x8 slice.
Arguments:
- x_in: bfloat16 [512, 4096], P('dp'), parts along dimension 0
- lengths: int32 [512], P('dp'), parts along dimension 0
- norm_gain: bfloat16 [2, 4096], replicated
- w_q: bfloat16 [2, 4096, 4096], P(None, None, 'tp')
- w_k: bfloat16 [2, 4096, 4096], P(None, None, 'tp')
- w_v: bfloat16 [2, 4096, 4096], P(None, None, 'tp')
- w_o: bfloat16 [2, 4096, 4096], P(None, 'tp')
- w_gate: bfloat16 [2, 4096, 11008], P(None, None, 'tp')
- w_up: bfloat16 [2, 4096, 11008], P(None, None, 'tp')
- w_down: bfloat16 [2, 11008, 4096], P(None, 'tp')
- k_cache: bfloat16 [2, 512, 32, 32, 128], P(None, 'dp', None, 'tp'), parts along dimension 1
- v_cache: bfloat16 [2, 512, 32, 32, 128], P(None, 'dp', None, 'tp'), parts along dimension 1
Outputs:
- output: bfloat16 [512, 4096], P('dp'), parts along dimension 0
There are 4 independent parts. The reference program is written for one: setup_inputs(seed, part) draws one part's arguments, and reference() takes and returns one part's arrays. A program takes and returns all parts, laid end to end along the dimension named above; an argument that names none is the same for every part.
All inputs are finite; a program needn't handle non-finite values.
Results may differ from the reference program's by a relative error of at most 0.0174662.
Values are sent between devices in bfloat16 or wider.
A program may use at most 768 MiB of HBM per device.

```python
import math
import jax
import jax.numpy as jnp
from jax import lax

D = 4096
HEADS = 32
KV_HEADS = 32
FF = 11008
HEAD = 128
BATCH = 128
SEQ = 32
LAYERS = 2
ROPE_BASE = 500000
NORM_EPS = 1e-5
GROUP = HEADS // KV_HEADS
LOG_LEVELS = int(math.log2(SEQ)) + 1


def draw_lengths(len_key):
    exp_key, val_key, top_key = jax.random.split(len_key, 3)
    span_exp = jax.random.randint(exp_key, (BATCH,), 0, LOG_LEVELS)
    span_limit = jnp.minimum(jnp.left_shift(jnp.ones_like(span_exp), span_exp), SEQ - 1)
    drawn_len = 1 + jax.random.randint(val_key, (BATCH,), 0, span_limit)
    full_slot = jax.random.randint(top_key, (), 0, BATCH)
    return jnp.where(jnp.arange(BATCH) == full_slot, SEQ - 1, drawn_len).astype(jnp.int32)


def setup_inputs(seed: int = 0, part: int = 0) -> dict:
    base_key = jax.random.key(seed)
    shared_keys = jax.random.split(base_key, 8)
    own_keys = jax.random.split(jax.random.fold_in(base_key, part), 4)
    q_width = HEADS * HEAD
    kv_width = KV_HEADS * HEAD

    def draw_weight(key_index, arr_shape, std_scale):
        return (jax.random.normal(shared_keys[key_index], arr_shape, jnp.float32) * std_scale).astype(jnp.bfloat16)

    return {
        'x_in': jax.random.normal(own_keys[0], (BATCH, D), jnp.float32).astype(jnp.bfloat16),
        'lengths': draw_lengths(own_keys[1]),
        'norm_gain': (1.0 + 0.3 * jax.random.normal(shared_keys[0], (LAYERS, D), jnp.float32)).astype(jnp.bfloat16),
        'w_q': draw_weight(1, (LAYERS, D, q_width), D ** -0.5),
        'w_k': draw_weight(2, (LAYERS, D, kv_width), 2.0 * D ** -0.5),
        'w_v': draw_weight(3, (LAYERS, D, kv_width), D ** -0.5),
        'w_o': draw_weight(4, (LAYERS, q_width, D), 2.0 * q_width ** -0.5),
        'w_gate': draw_weight(5, (LAYERS, D, FF), D ** -0.5),
        'w_up': draw_weight(6, (LAYERS, D, FF), D ** -0.5),
        'w_down': draw_weight(7, (LAYERS, FF, D), FF ** -0.5),
        'k_cache': (2.0 * jax.random.normal(own_keys[2], (LAYERS, BATCH, SEQ, KV_HEADS, HEAD), jnp.float32)).astype(jnp.bfloat16),
        'v_cache': jax.random.normal(own_keys[3], (LAYERS, BATCH, SEQ, KV_HEADS, HEAD), jnp.float32).astype(jnp.bfloat16),
    }


def rms_norm(x_res, gain_row):
    x_f32 = x_res.astype(jnp.float32)
    inv_rms = lax.rsqrt(jnp.mean(x_f32 * x_f32, axis=-1, keepdims=True) + NORM_EPS)
    return (x_f32 * inv_rms * gain_row.astype(jnp.float32)).astype(jnp.bfloat16)


def rope_rotate(head_vecs, positions):
    half_dim = HEAD // 2
    inv_freq = 1.0 / (ROPE_BASE ** (jnp.arange(0, HEAD, 2).astype(jnp.float32) / HEAD))
    angles = positions.astype(jnp.float32)[:, None] * inv_freq[None, :]
    cos_ang = jnp.cos(angles)[:, None, :]
    sin_ang = jnp.sin(angles)[:, None, :]
    vec_f32 = head_vecs.astype(jnp.float32)
    rot_first = vec_f32[..., :half_dim]
    rot_second = vec_f32[..., half_dim:]
    return jnp.concatenate([rot_first * cos_ang - rot_second * sin_ang, rot_second * cos_ang + rot_first * sin_ang], axis=-1).astype(jnp.bfloat16)


def decode_attention(q_rot, k_rot, v_new, k_layer, v_layer, lengths):
    attn_scale = HEAD ** -0.5
    q_f32 = q_rot.astype(jnp.float32)
    cache_logits = jnp.einsum('bkgd,bskd->bkgs', q_f32, k_layer.astype(jnp.float32)) * attn_scale
    valid_mask = jnp.arange(SEQ)[None, :] < lengths[:, None]
    cache_logits = jnp.where(valid_mask[:, None, None, :], cache_logits, -jnp.inf)
    self_logit = jnp.einsum('bkgd,bkd->bkg', q_f32, k_rot.astype(jnp.float32)) * attn_scale
    row_peak = jnp.maximum(jnp.max(cache_logits, axis=-1), self_logit)
    cache_w = jnp.exp(cache_logits - row_peak[..., None])
    self_w = jnp.exp(self_logit - row_peak)
    prob_denom = jnp.sum(cache_w, axis=-1) + self_w
    cache_p = (cache_w / prob_denom[..., None]).astype(jnp.bfloat16)
    self_p = (self_w / prob_denom).astype(jnp.bfloat16)
    cache_part = jnp.einsum('bkgs,bskd->bkgd', cache_p.astype(jnp.float32), v_layer.astype(jnp.float32))
    self_part = self_p.astype(jnp.float32)[..., None] * v_new.astype(jnp.float32)[:, :, None, :]
    return (cache_part + self_part).astype(jnp.bfloat16)


def reference(x_in, lengths, norm_gain, w_q, w_k, w_v, w_o, w_gate, w_up, w_down, k_cache, v_cache):
    def layer_step(x_res, layer_args):
        gain_row, wq_layer, wk_layer, wv_layer, wo_layer, wg_layer, wu_layer, wd_layer, k_layer, v_layer = layer_args
        normed = rms_norm(x_res, gain_row)
        q_proj = jnp.dot(normed, wq_layer, preferred_element_type=jnp.float32).astype(jnp.bfloat16).reshape(BATCH, HEADS, HEAD)
        k_proj = jnp.dot(normed, wk_layer, preferred_element_type=jnp.float32).astype(jnp.bfloat16).reshape(BATCH, KV_HEADS, HEAD)
        v_new = jnp.dot(normed, wv_layer, preferred_element_type=jnp.float32).astype(jnp.bfloat16).reshape(BATCH, KV_HEADS, HEAD)
        q_rot = rope_rotate(q_proj, lengths).reshape(BATCH, KV_HEADS, GROUP, HEAD)
        k_rot = rope_rotate(k_proj, lengths)
        attn_flat = decode_attention(q_rot, k_rot, v_new, k_layer, v_layer, lengths).reshape(BATCH, HEADS * HEAD)
        attn_proj = jnp.dot(attn_flat, wo_layer, preferred_element_type=jnp.float32)
        gate_act = jnp.dot(normed, wg_layer, preferred_element_type=jnp.float32).astype(jnp.bfloat16)
        up_act = jnp.dot(normed, wu_layer, preferred_element_type=jnp.float32).astype(jnp.bfloat16)
        mlp_hidden = (jax.nn.silu(gate_act.astype(jnp.float32)) * up_act.astype(jnp.float32)).astype(jnp.bfloat16)
        mlp_proj = jnp.dot(mlp_hidden, wd_layer, preferred_element_type=jnp.float32)
        x_next = (x_res.astype(jnp.float32) + attn_proj + mlp_proj).astype(jnp.bfloat16)
        return x_next, None

    scan_result = lax.scan(layer_step, x_in, (norm_gain, w_q, w_k, w_v, w_o, w_gate, w_up, w_down, k_cache, v_cache))
    return scan_result[0]
```

```python
import functools

import numpy as np
import jax
import jax.numpy as jnp
from jax import lax
from jax.experimental import pallas as pl
from jax.experimental.pallas import tpu as pltpu
from jax.sharding import PartitionSpec as P

NORM_EPS = 1e-5
ROPE_BASE = 500000.0
F32 = jnp.float32
BF16 = jnp.bfloat16
AHEAD = 6
NSUB = 2
LAG = 3


def decode_kernel(cfg, x_hbm, len_ref, freq_ref, gain_ref, wq_hbm, wk_hbm, wv_hbm, wo_hbm, wg_hbm, wu_hbm, wd_hbm,
                  kc_hbm, vc_hbm, out_hbm,
                  xg, wqkv, wg, wu, wod, kbuf, vbuf, gain_s, rb, lenb, cosb, sinb, acc_qkv, acc_g, acc_u, ut,
                  qs, ks, vs, logit_s, prob_s, hbuf, attn_s, own_f, snd_f, rcv_f, shr_snd, shr_rcv, stats,
                  x_sem, w_sem, kv_sem, od_sem, pair_s_sem, pair_r_sem, rs_s_sem, rs_r_sem, st_s_sem, st_r_sem,
                  ag_s_sem, ag_l_sem, ag_r_sem, pf_s_sem, pf_r_sem, out_sem):
    tp, rows, width, ff, seq, head, hq, layers = cfg
    chips = tp // 2
    half = chips // 2
    cw = width // tp
    me = lax.axis_index("tp")
    z = me // 2
    c = lax.rem(me, 2)
    partner = z * 2 + (1 - c)
    scale = head ** -0.5
    nch = tp
    nqkv = 3 * cw
    grp = 8
    ngrp = rows // grp
    gcols = grp * seq * hq

    def ring_dev(off):
        return lax.rem(z + off + chips, chips) * 2 + c

    def x_copy(k):
        return pltpu.make_async_copy(x_hbm.at[:, pl.ds(k * cw, cw)], xg.at[0, k], x_sem.at[k])

    def w_copies(l, k):
        r = pl.ds(k * cw, cw)
        return [
            pltpu.make_async_copy(wq_hbm.at[l, r, :], wqkv.at[k, :, 0:cw], w_sem.at[k, 0]),
            pltpu.make_async_copy(wk_hbm.at[l, r, :], wqkv.at[k, :, cw:2 * cw], w_sem.at[k, 1]),
            pltpu.make_async_copy(wv_hbm.at[l, r, :], wqkv.at[k, :, 2 * cw:3 * cw], w_sem.at[k, 2]),
            pltpu.make_async_copy(wg_hbm.at[l, :, r], wg.at[k], w_sem.at[k, 3]),
            pltpu.make_async_copy(wu_hbm.at[l, :, r], wu.at[k], w_sem.at[k, 4]),
        ]

    def kv_copies(l):
        return [pltpu.make_async_copy(kc_hbm.at[l], kbuf, kv_sem.at[0]), pltpu.make_async_copy(vc_hbm.at[l], vbuf, kv_sem.at[1])]

    def od_copies(l, j):
        cs = pl.ds(j * 2 * cw, 2 * cw)
        return [
            pltpu.make_async_copy(wo_hbm.at[l, :, cs], wod.at[j, 0:cw, :], od_sem.at[j, 0]),
            pltpu.make_async_copy(wd_hbm.at[l, :, cs], wod.at[j, cw:cw + ff, :], od_sem.at[j, 1]),
        ]

    def start(cps):
        for cp in cps:
            cp.start()

    def wait(cps):
        for cp in cps:
            cp.wait()

    sends = []

    def send(src, dst, s_sem, r_sem, dev):
        cp = pltpu.make_async_remote_copy(src_ref=src, dst_ref=dst, send_sem=s_sem, recv_sem=r_sem,
                                          device_id={"tp": dev}, device_id_type=pl.DeviceIdType.MESH)
        cp.start()
        sends.append(cp)

    def wait_recv(dst, r_sem):
        pltpu.make_async_remote_copy(src_ref=dst, dst_ref=dst, send_sem=r_sem, recv_sem=r_sem, device_id={"tp": partner}, device_id_type=pl.DeviceIdType.MESH).wait_recv()

    for k in range(nch):
        x_copy(k).start()
    for k in range(AHEAD):
        start(w_copies(0, k))

    barrier = pltpu.get_barrier_semaphore()
    for d in range(1, tp):
        pl.semaphore_signal(barrier, inc=1, device_id={"tp": lax.rem(me + d, tp)}, device_id_type=pl.DeviceIdType.MESH)

    pad = wod.shape[1] - cw - ff
    if pad:
        for j in range(chips):
            wod[j, cw + ff:, :] = jnp.zeros((pad, 2 * cw), BF16)
        ut[ff:, :] = jnp.zeros((pad, rows), F32)
    gain_s[...] = gain_ref[...].astype(F32)
    lenb[...] = jnp.broadcast_to(len_ref[...].astype(F32), (rows, rows)).T
    ang = lenb[...] * freq_ref[...]
    lane = lax.broadcasted_iota(jnp.int32, (rows, head), 1)
    cosb[...] = jnp.cos(ang)
    sn = jnp.sin(ang)
    sinb[...] = jnp.where(lane < head // 2, -sn, sn)

    def set_inv_rms(ssq):
        inv = lax.rsqrt(ssq / width + NORM_EPS)
        rb[...] = jnp.broadcast_to(inv, rb.shape)

    def do_chunk(l, k):
        xk = xg[l, k].astype(F32)
        g = gain_s[l:l + 1, pl.ds(pl.multiple_of(k * cw, cw), cw)]
        a = (xk * rb[...] * g).astype(BF16)
        acc_qkv[...] += jnp.dot(a, wqkv[k], preferred_element_type=F32)
        nt = (((1,), (1,)), ((), ()))
        acc_g[...] += lax.dot_general(wg[k], a, nt, preferred_element_type=F32)
        acc_u[...] += lax.dot_general(wu[k], a, nt, preferred_element_type=F32)

    def rope(v):
        return (v * cosb[...] + pltpu.roll(v, head // 2, 1) * sinb[...]).astype(BF16).astype(F32)

    def zero_acc():
        acc_qkv[...] = jnp.zeros_like(acc_qkv)
        acc_g[...] = jnp.zeros_like(acc_g)
        acc_u[...] = jnp.zeros_like(acc_u)

    def attention(l):
        for h in range(hq):
            q = acc_qkv[:, h * head:(h + 1) * head].astype(BF16).astype(F32)
            k = acc_qkv[:, cw + h * head:cw + (h + 1) * head].astype(BF16).astype(F32)
            v = acc_qkv[:, 2 * cw + h * head:2 * cw + (h + 1) * head].astype(BF16).astype(F32)
            qs[:, h] = rope(q).reshape(ngrp, grp, head)
            ks[:, h] = rope(k).reshape(ngrp, grp, head)
            vs[:, h] = v.reshape(ngrp, grp, head)
        wait(kv_copies(l))
        m = hq * grp
        for g in range(ngrp):
            q = qs[g].reshape(m, head).astype(BF16)
            kk = kbuf[g * gcols:(g + 1) * gcols, :]
            logit_s[g * m:(g + 1) * m, :] = lax.dot_general(q, kk, (((1,), (1,)), ((), ())), preferred_element_type=F32)
        col = lax.broadcasted_iota(jnp.int32, (m, gcols), 1)
        row = lax.broadcasted_iota(jnp.int32, (m, gcols), 0)
        same = ((col // (seq * hq)) == lax.rem(row, grp)) & (lax.rem(col, hq) == row // grp)
        key = jnp.where(same, lax.rem(col // hq, seq), 2 * seq).astype(F32)
        for g in range(ngrp):
            ln = lenb[g * grp:(g + 1) * grp, 0:1]
            ln = jnp.concatenate([ln] * hq, axis=0)
            lg = jnp.where(key < ln, logit_s[g * m:(g + 1) * m, :] * scale, -jnp.inf)
            qv = qs[g].reshape(m, head)
            kv = ks[g].reshape(m, head)
            vv = vs[g].reshape(m, head)
            sl = jnp.sum(qv * kv, axis=1, keepdims=True) * scale
            peak = jnp.maximum(jnp.max(lg, axis=1, keepdims=True), sl)
            w = jnp.exp(lg - peak)
            sw = jnp.exp(sl - peak)
            den = jnp.sum(w, axis=1, keepdims=True) + sw
            prob_s[g * m:(g + 1) * m, :] = (w / den).astype(BF16)
            sp = (sw / den).astype(BF16).astype(F32)
            vs[g] = (sp * vv).reshape(hq, grp, head)
        for g in range(ngrp):
            p = prob_s[g * m:(g + 1) * m, :]
            o = jnp.dot(p, vbuf[g * gcols:(g + 1) * gcols, :], preferred_element_type=F32)
            o = o + vs[g].reshape(m, head)
            for h in range(hq):
                attn_s[g * grp:(g + 1) * grp, h * head:(h + 1) * head] = o[h * grp:(h + 1) * grp]
        hbuf[:, 0:cw] = attn_s[...].astype(BF16)

    def mlp_act():
        gt = acc_g[...].astype(BF16).astype(F32)
        up = acc_u[...].astype(BF16).astype(F32)
        ut[0:ff, :] = gt * (1.0 / (1.0 + jnp.exp(-gt))) * up
        for i in range(ut.shape[0] // 128):
            hbuf[:, cw + i * 128:cw + (i + 1) * 128] = ut[i * 128:(i + 1) * 128, :].T.astype(BF16)

    offs = [half]
    for d in range(half - 1, 0, -1):
        offs += [d, chips - d]
    offs += [0]

    def out_proj(l):
        hv = hbuf[...]

        def finish(i):
            off = offs[i]
            wait_recv(rcv_f.at[l, i], pair_r_sem.at[l, i])
            s = own_f[l, i] + rcv_f[l, i]
            if off == 0:
                own_f[l, i] = s
            else:
                shr_snd[l, i] = s.astype(BF16)
                send(shr_snd.at[l, i], shr_rcv.at[l, i], rs_s_sem.at[l, i], rs_r_sem.at[l, i], ring_dev(off))

        for i in range(chips):
            j = lax.rem(z + offs[i], chips)
            wait(od_copies(l, j))
            p = jnp.dot(hv, wod[j], preferred_element_type=F32)
            lo, hi = p[:, :cw], p[:, cw:]
            own_f[l, i] = jnp.where(c == 0, lo, hi)
            snd_f[l, i] = jnp.where(c == 0, hi, lo)
            send(snd_f.at[l, i], rcv_f.at[l, i], pair_s_sem.at[l, i], pair_r_sem.at[l, i], partner)
            if i >= LAG:
                finish(i - LAG)
        for i in range(chips - LAG, chips):
            finish(i)

    def reduce_own(l):
        acc = xg[l, me].astype(F32) + own_f[l, chips - 1]
        for i in range(chips - 1):
            wait_recv(shr_rcv.at[l, i], rs_r_sem.at[l, i])
            acc = acc + shr_rcv[l, i].astype(F32)
        return acc.astype(BF16)

    pr = rows // NSUB

    def gather(l, use):
        dst = l + 1

        def piece(src, p):
            return xg.at[dst, src, pl.ds(p * pr, pr), :]

        def to_partner(src, q, p):
            send(piece(src, p), piece(src, p), pf_s_sem.at[l, q, p], pf_r_sem.at[l, q, p], partner)

        def ring(src, step, p, right):
            dev = ring_dev(1 if right else -1)
            r = (ag_l_sem if right else ag_r_sem).at[l, step, p]
            send(piece(src, p), piece(src, p), ag_s_sem.at[l, step, 0 if right else 1, p], r, dev)

        for p in range(NSUB):
            ring(me, 0, p, True)
            ring(me, 0, p, False)
        for p in range(NSUB):
            to_partner(me, 0, p)
        use("own", [me])
        for s in range(1, half):
            sl, sr = ring_dev(-s), ring_dev(s)
            for p in range(NSUB):
                wait_recv(piece(sl, p), ag_l_sem.at[l, s - 1, p])
                if s < half - 1 or p < NSUB // 2:
                    ring(sl, s, p, True)
                to_partner(sl, 2 * s - 1, p)
                wait_recv(piece(sr, p), ag_r_sem.at[l, s - 1, p])
                if s < half - 1 or p >= NSUB // 2:
                    ring(sr, s, p, False)
                to_partner(sr, 2 * s, p)
            use("ring", [sl, sr])
            flip = 1 - 2 * c
            qs_ = [0] if s == 1 else [2 * s - 3, 2 * s - 2]
            srcs = [me + flip] if s == 1 else [ring_dev(1 - s) + flip, ring_dev(s - 1) + flip]
            for q, src in zip(qs_, srcs):
                for p in range(NSUB):
                    wait_recv(piece(src, p), pf_r_sem.at[l, q, p])
            use("pair", srcs)
        far = ring_dev(half)
        for p in range(NSUB // 2):
            wait_recv(piece(far, p), ag_l_sem.at[l, half - 1, p])
            to_partner(far, 2 * half - 1, p)
            p2 = p + NSUB // 2
            wait_recv(piece(far, p2), ag_r_sem.at[l, half - 1, p2])
            to_partner(far, 2 * half - 1, p2)
        use("ring", [far])
        flip = 1 - 2 * c
        for q, src in ((2 * half - 3, ring_dev(1 - half) + flip), (2 * half - 2, ring_dev(half - 1) + flip), (2 * half - 1, far + flip)):
            for p in range(NSUB):
                wait_recv(piece(src, p), pf_r_sem.at[l, q, p])
            use("pair", [src])

    ssq = jnp.zeros((rows, cw), F32)
    for k in range(nch):
        x_copy(k).wait()
        xf = xg[0, k].astype(F32)
        ssq = ssq + xf * xf
    set_inv_rms(jnp.sum(ssq, axis=1, keepdims=True))
    zero_acc()

    def l0_body(k, carry):
        wait(w_copies(0, k))
        do_chunk(0, k)

        @pl.when(k + AHEAD < nch)
        def _():
            start(w_copies(0, k + AHEAD))

        @pl.when(k + AHEAD == nch)
        def _():
            start(kv_copies(0))
            for i in range(chips):
                start(od_copies(0, lax.rem(z + offs[i], chips)))
        return carry

    lax.fori_loop(0, nch, l0_body, 0)

    for l in range(layers):
        attention(l)
        mlp_act()
        if l == 0:
            pl.semaphore_wait(barrier, tp - 1)
        out_proj(l)
        if l + 1 < layers:
            for k in range(nch):
                start(w_copies(l + 1, k))
            start(kv_copies(l + 1))
            for i in range(chips):
                start(od_copies(l + 1, lax.rem(z + offs[i], chips)))
        xn = reduce_own(l)
        xg[l + 1, me] = xn
        if l + 1 < layers:
            xf = xn.astype(F32)
            sq = jnp.sum(xf * xf, axis=1, keepdims=True)
            stats[l, me] = jnp.broadcast_to(sq, (rows, rows)).T[0:8, :]

            def use(kind, srcs, l=l):
                if kind == "own":
                    for d in range(1, tp):
                        send(stats.at[l, me], stats.at[l, me], st_s_sem.at[l, d], st_r_sem.at[l, me], lax.rem(me + d, tp))
                    zero_acc()
                    wait_all_w = w_copies
                    return
                if kind == "ring" and not use.ready:
                    use.ready = True
                    for d in range(1, tp):
                        o = lax.rem(me + d, tp)
                        wait_recv(stats.at[l, o], st_r_sem.at[l, o])
                    tot = stats[l, 0]
                    for d in range(1, tp):
                        tot = tot + stats[l, d]
                    set_inv_rms(jnp.broadcast_to(tot[0:1, :], (rows, rows)).T[:, 0:1])
                    srcs = [me] + srcs
                for src in srcs:
                    wait(w_copies(l + 1, src))
                    do_chunk(l + 1, src)

            use.ready = False
            gather(l, use)
        else:
            outs = []

            def use_out(kind, srcs, l=l):
                for src in srcs:
                    cp = pltpu.make_async_copy(xg.at[l + 1, src], out_hbm.at[:, pl.ds(pl.multiple_of(src * cw, cw), cw)], out_sem.at[src])
                    cp.start()
                    outs.append(cp)

            gather(l, use_out)
            wait(outs)
    for cp in sends:
        cp.wait_send()


def solution(mesh):
    tp = mesh.shape["tp"]
    arg_specs = (P("dp", None), P("dp"), P(), P(None, None, "tp"), P(None, None, "tp"), P(None, None, "tp"), P(None, "tp", None),
                 P(None, None, "tp"), P(None, None, "tp"), P(None, "tp", None), P(None, "dp", None, "tp", None), P(None, "dp", None, "tp", None))

    def per_device(x_in, lengths, norm_gain, w_q, w_k, w_v, w_o, w_gate, w_up, w_down, k_cache, v_cache):
        rows, width = x_in.shape
        layers, _, seq, hq, head = k_cache.shape
        ff = w_gate.shape[2]
        cw = width // tp
        chips = tp // 2
        assert w_q.shape[2] == cw == hq * head
        freq = (1.0 / (np.float32(ROPE_BASE) ** (np.arange(0, head, 2).astype(np.float32) / np.float32(head)))).astype(np.float32)
        freq = jnp.asarray(np.concatenate([freq, freq])[None, :])
        ffp = -(-(cw + ff) // 256) * 256 - cw
        kvr = rows * seq * hq
        ngrp = rows // 8
        m = hq * 8
        any_spec = pl.BlockSpec(memory_space=pl.ANY)
        vmem = pl.BlockSpec(memory_space=pltpu.VMEM)
        V = pltpu.VMEM
        D = pltpu.SemaphoreType.DMA
        scratch = [
            V((layers + 1, tp, rows, cw), BF16),
            V((tp, cw, 3 * cw), BF16),
            V((tp, ff, cw), BF16), V((tp, ff, cw), BF16),
            V((chips, cw + ffp, 2 * cw), BF16),
            V((kvr, head), BF16), V((kvr, head), BF16),
            V((layers, width), F32),
            V((rows, cw), F32),
            V((rows, rows), F32),
            V((rows, head), F32), V((rows, head), F32),
            V((rows, 3 * cw), F32),
            V((ff, rows), F32), V((ff, rows), F32),
            V((ffp, rows), F32),
            V((ngrp, hq, 8, head), F32), V((ngrp, hq, 8, head), F32), V((ngrp, hq, 8, head), F32),
            V((rows * hq, 8 * seq * hq), F32),
            V((rows * hq, 8 * seq * hq), BF16),
            V((rows, cw + ffp), BF16),
            V((rows, cw), F32),
            V((layers, chips, rows, cw), F32),
            V((layers, chips, rows, cw), F32),
            V((layers, chips, rows, cw), F32),
            V((layers, chips, rows, cw), BF16),
            V((layers, chips, rows, cw), BF16),
            V((layers, tp, 8, rows), F32),
            D((tp,)), D((tp, 5)), D((2,)), D((chips, 2)),
            D((layers, chips)), D((layers, chips)), D((layers, chips)), D((layers, chips)),
            D((layers, tp)), D((layers, tp)),
            D((layers, chips // 2, 2, NSUB)), D((layers, chips // 2, NSUB)), D((layers, chips // 2, NSUB)),
            D((layers, chips, NSUB)), D((layers, chips, NSUB)), D((tp,)),
        ]
        cfg = (tp, rows, width, ff, seq, head, hq, layers)
        return pl.pallas_call(
            functools.partial(decode_kernel, cfg),
            out_shape=jax.ShapeDtypeStruct((rows, width), BF16),
            in_specs=[any_spec, vmem, vmem, vmem] + [any_spec] * 9,
            out_specs=any_spec,
            scratch_shapes=scratch,
            compiler_params=pltpu.CompilerParams(collective_id=0, has_side_effects=True, vmem_limit_bytes=60 * 1024 * 1024),
        )(x_in, lengths.reshape(1, rows), freq, norm_gain, w_q, w_k, w_v, w_o, jnp.swapaxes(w_gate, 1, 2), jnp.swapaxes(w_up, 1, 2), w_down,
          k_cache.reshape(layers, kvr, head), v_cache.reshape(layers, kvr, head))

    return jax.shard_map(per_device, mesh=mesh, in_specs=arg_specs, out_specs=P("dp", None), check_vma=False)
```

```python
import functools

import numpy as np
import jax
import jax.numpy as jnp
from jax import lax
from jax.experimental import pallas as pl
from jax.experimental.pallas import tpu as pltpu
from jax.sharding import PartitionSpec as P

NORM_EPS = 1e-5
ROPE_BASE = 500000.0
F32 = jnp.float32
BF16 = jnp.bfloat16
NSUB = 2
LAG = 3
FIRST = 2
AHEAD = 7
RING = 8


def decode_kernel(cfg, x_hbm, len_ref, freq_ref, gain_ref, wq_hbm, wk_hbm, wv_hbm, wo_hbm, wg_hbm, wu_hbm, wd_hbm,
                  kc_hbm, vc_hbm, out_hbm,
                  xg, wqkv, wgu, wod, kbuf, vbuf, gain_s, rb, lenb, cosb, sinb, acc_qkv, acc_g, acc_u, ut,
                  qs, ks, vs, logit_s, prob_s, hbuf, attn_s, own_f, snd_f, rcv_f, shr_snd, shr_rcv, stats,
                  x_sem, w_sem, wl_sem, kv_sem, od_sem, pair_s_sem, pair_r_sem, rs_s_sem, rs_r_sem, st_s_sem, st_r_sem,
                  ag_s_sem, ag_r_sem, pf_r_sem, out_sem):
    tp, rows, width, ff, seq, head, hq, layers = cfg
    chips = tp // 2
    half = chips // 2
    cw = width // tp
    me = lax.axis_index("tp")
    z = me // 2
    c = lax.rem(me, 2)
    partner = z * 2 + (1 - c)
    scale = head ** -0.5
    nch = tp
    nqkv = 3 * cw
    grp = 8
    ngrp = rows // grp
    gcols = grp * seq * hq

    def ring_dev(off):
        return lax.rem(z + off + chips, chips) * 2 + c

    def x_copy(k):
        return pltpu.make_async_copy(x_hbm.at[:, pl.ds(k * cw, cw)], xg.at[0, k], x_sem)

    def start_w(l, k, qkv_sem, gu_sem):
        r = pl.ds(k * cw, cw)
        for i, w in enumerate((wq_hbm, wk_hbm, wv_hbm)):
            pltpu.make_async_copy(w.at[l, r, :], wqkv.at[k, :, i * cw:(i + 1) * cw], qkv_sem).start()
        for i, w in enumerate((wg_hbm, wu_hbm)):
            pltpu.make_async_copy(w.at[l, :, r], wgu.at[k, i], gu_sem).start()

    def start_kv(l):
        pltpu.make_async_copy(kc_hbm.at[l], kbuf, kv_sem.at[0]).start()
        pltpu.make_async_copy(vc_hbm.at[l], vbuf, kv_sem.at[1]).start()

    def start_od(l, j):
        cs = pl.ds(j * 2 * cw, 2 * cw)
        pltpu.make_async_copy(wo_hbm.at[l, :, cs], wod.at[j, 0:cw, :], od_sem).start()
        pltpu.make_async_copy(wd_hbm.at[l, :, cs], wod.at[j, cw:cw + ff, :], od_sem).start()

    def start_all_od(l):
        for i in range(chips):
            start_od(l, lax.rem(z + offs[i], chips))

    def arrive(ref, sem):
        pltpu.make_async_copy(ref, ref, sem).wait()

    def send(src, dst, s_sem, r_sem, dev):
        cp = pltpu.make_async_remote_copy(src_ref=src, dst_ref=dst, send_sem=s_sem, recv_sem=r_sem,
                                          device_id={"tp": dev}, device_id_type=pl.DeviceIdType.MESH)
        cp.start()

    def wait_remote(dst, sem):
        return pltpu.make_async_remote_copy(src_ref=dst, dst_ref=dst, send_sem=sem, recv_sem=sem,
                                            device_id={"tp": partner}, device_id_type=pl.DeviceIdType.MESH)

    def wait_recv(dst, sem):
        wait_remote(dst, sem).wait_recv()

    def wait_sent(src, sem):
        wait_remote(src, sem).wait_send()

    offs = [half]
    for d in range(half - 1, 0, -1):
        offs += [d, chips - d]
    offs += [0]
    for k in range(nch):
        x_copy(k).start()
    for k in range(FIRST):
        start_w(0, k, w_sem.at[k, 0], w_sem.at[k, 1])

    scope_pre = jax.named_scope("pre")
    scope_pre.__enter__()
    barrier = pltpu.get_barrier_semaphore()
    for d in range(1, tp):
        pl.semaphore_signal(barrier, inc=1, device_id={"tp": lax.rem(me + d, tp)}, device_id_type=pl.DeviceIdType.MESH)

    pad = wod.shape[1] - cw - ff
    if pad:
        for j in range(chips):
            wod[j, cw + ff:, :] = jnp.zeros((pad, 2 * cw), BF16)
        ut[ff:, :] = jnp.zeros((pad, rows), F32)
    gain_s[...] = gain_ref[...].astype(F32)
    lenb[...] = jnp.broadcast_to(len_ref[...].astype(F32), (rows, rows)).T
    ang = lenb[...] * freq_ref[...]
    lane = lax.broadcasted_iota(jnp.int32, (rows, head), 1)
    cosb[...] = jnp.cos(ang)
    sn = jnp.sin(ang)
    sinb[...] = jnp.where(lane < head // 2, -sn, sn)
    scope_pre.__exit__(None, None, None)

    def set_inv_rms(ssq):
        inv = lax.rsqrt(ssq / width + NORM_EPS)
        rb[...] = jnp.broadcast_to(inv, rb.shape)

    def do_chunk(l, k):
        xk = xg[l, k].astype(F32)
        g = gain_s[l:l + 1, pl.ds(pl.multiple_of(k * cw, cw), cw)]
        a = (xk * rb[...] * g).astype(BF16)
        acc_qkv[...] += jnp.dot(a, wqkv[k], preferred_element_type=F32)
        nt = (((1,), (1,)), ((), ()))
        acc_g[...] += lax.dot_general(wgu[k, 0], a, nt, preferred_element_type=F32)
        acc_u[...] += lax.dot_general(wgu[k, 1], a, nt, preferred_element_type=F32)

    def rope(v):
        return (v * cosb[...] + pltpu.roll(v, head // 2, 1) * sinb[...]).astype(BF16).astype(F32)

    def zero_acc():
        acc_qkv[...] = jnp.zeros_like(acc_qkv)
        acc_g[...] = jnp.zeros_like(acc_g)
        acc_u[...] = jnp.zeros_like(acc_u)

    def attention(l):
        for h in range(hq):
            q = acc_qkv[:, h * head:(h + 1) * head].astype(BF16).astype(F32)
            k = acc_qkv[:, cw + h * head:cw + (h + 1) * head].astype(BF16).astype(F32)
            v = acc_qkv[:, 2 * cw + h * head:2 * cw + (h + 1) * head].astype(BF16).astype(F32)
            qs[:, h] = rope(q).reshape(ngrp, grp, head)
            ks[:, h] = rope(k).reshape(ngrp, grp, head)
            vs[:, h] = v.reshape(ngrp, grp, head)
        with jax.named_scope(f"kvwait{l}"):
            arrive(kbuf, kv_sem.at[0])
            arrive(vbuf, kv_sem.at[1])
        m = hq * grp
        for g in range(ngrp):
            q = qs[g].reshape(m, head).astype(BF16)
            kk = kbuf[g * gcols:(g + 1) * gcols, :]
            logit_s[g * m:(g + 1) * m, :] = lax.dot_general(q, kk, (((1,), (1,)), ((), ())), preferred_element_type=F32)
        col = lax.broadcasted_iota(jnp.int32, (m, gcols), 1)
        row = lax.broadcasted_iota(jnp.int32, (m, gcols), 0)
        same = ((col // (seq * hq)) == lax.rem(row, grp)) & (lax.rem(col, hq) == row // grp)
        key = jnp.where(same, lax.rem(col // hq, seq), 2 * seq).astype(F32)
        for g in range(ngrp):
            ln = lenb[g * grp:(g + 1) * grp, 0:1]
            ln = jnp.concatenate([ln] * hq, axis=0)
            lg = jnp.where(key < ln, logit_s[g * m:(g + 1) * m, :] * scale, -jnp.inf)
            qv = qs[g].reshape(m, head)
            kv = ks[g].reshape(m, head)
            vv = vs[g].reshape(m, head)
            sl = jnp.sum(qv * kv, axis=1, keepdims=True) * scale
            peak = jnp.maximum(jnp.max(lg, axis=1, keepdims=True), sl)
            w = jnp.exp(lg - peak)
            sw = jnp.exp(sl - peak)
            den = jnp.sum(w, axis=1, keepdims=True) + sw
            prob_s[g * m:(g + 1) * m, :] = (w / den).astype(BF16)
            sp = (sw / den).astype(BF16).astype(F32)
            vs[g] = (sp * vv).reshape(hq, grp, head)
        for g in range(ngrp):
            p = prob_s[g * m:(g + 1) * m, :]
            o = jnp.dot(p, vbuf[g * gcols:(g + 1) * gcols, :], preferred_element_type=F32)
            o = o + vs[g].reshape(m, head)
            for h in range(hq):
                attn_s[g * grp:(g + 1) * grp, h * head:(h + 1) * head] = o[h * grp:(h + 1) * grp]
        hbuf[:, 0:cw] = attn_s[...].astype(BF16)

    def mlp_act():
        gt = acc_g[...].astype(BF16).astype(F32)
        up = acc_u[...].astype(BF16).astype(F32)
        ut[0:ff, :] = gt * (1.0 / (1.0 + jnp.exp(-gt))) * up
        for i in range(ut.shape[0] // 128):
            hbuf[:, cw + i * 128:cw + (i + 1) * 128] = ut[i * 128:(i + 1) * 128, :].T.astype(BF16)

    def out_proj(l):
        arrive(wod.at[:, 0:cw + ff, :], od_sem)
        hv = hbuf[...]

        def finish(i):
            off = offs[i]
            wait_recv(rcv_f.at[l, i], pair_r_sem.at[i])
            s = own_f[l, i] + rcv_f[l, i]
            if off == 0:
                own_f[l, i] = s
            else:
                shr_snd[l, i] = s.astype(BF16)
                send(shr_snd.at[l, i], shr_rcv.at[l, i], rs_s_sem, rs_r_sem.at[i], ring_dev(off))

        for i in range(chips):
            j = lax.rem(z + offs[i], chips)
            p = jnp.dot(hv, wod[j], preferred_element_type=F32)
            lo, hi = p[:, :cw], p[:, cw:]
            own_f[l, i] = jnp.where(c == 0, lo, hi)
            snd_f[l, i] = jnp.where(c == 0, hi, lo)
            send(snd_f.at[l, i], rcv_f.at[l, i], pair_s_sem, pair_r_sem.at[i], partner)
            if i >= LAG:
                finish(i - LAG)
        for i in range(chips - LAG, chips):
            finish(i)
        wait_sent(snd_f.at[l], pair_s_sem)

    def reduce_own(l):
        acc = xg[l, me].astype(F32) + own_f[l, chips - 1]
        for i in range(chips - 1):
            wait_recv(shr_rcv.at[l, i], rs_r_sem.at[i])
            acc = acc + shr_rcv[l, i].astype(F32)
        wait_sent(shr_snd.at[l, 0:chips - 1], rs_s_sem)
        return acc.astype(BF16)

    pr = rows // NSUB

    def gather(l, use):
        dst = l + 1
        flip = 1 - 2 * c
        first, last = list(range(NSUB)), list(range(NSUB))[::-1]

        def piece(src, p):
            return xg.at[dst, src, pl.ds(p * pr, pr), :]

        def whole(src):
            return xg.at[dst, src]

        def slot(d, side):
            return 0 if d == 0 else (2 * half - 1 if d == half else 2 * d - 1 + side)

        def sem_of(d, side, p):
            return ag_r_sem.at[p * 2 + side] if d == 2 else ag_r_sem.at[2 * NSUB + (0 if d == half else (d // 2 + 1) * 2 - 1 + side)]

        def to_partner(ref, d, side):
            send(ref, ref, ag_s_sem, pf_r_sem.at[slot(d, side)], partner)

        def ring(ref, d, p, hops):
            send(ref, ref, ag_s_sem, sem_of(d, 0 if hops > 0 else 1, p), ring_dev(hops))

        def arrived(d, side):
            src = ring_dev(-d if side == 0 else d)
            wait_recv(whole(src), sem_of(d, side, 0))
            to_partner(whole(src), d, side)
            return src

        def from_partner(d, side):
            src = me + flip if d == 0 else ring_dev(-d if side == 0 else d) + flip
            wait_recv(whole(src), pf_r_sem.at[slot(d, side)])
            return src

        for i in range(NSUB):
            ring(piece(me, first[i]), 2, first[i], 2)
            ring(piece(me, last[i]), 2, last[i], -2)
        use("early", [])
        ring(whole(me), 1, 0, 1)
        ring(whole(me), 1, 0, -1)
        to_partner(whole(me), 0, 0)
        use("own", [me])
        two = [ring_dev(-2), ring_dev(2)]
        for i in range(NSUB):
            for side, p in ((0, first[i]), (1, last[i])):
                src = two[side]
                wait_recv(piece(src, p), sem_of(2, side, p))
                sg = 1 if side == 0 else -1
                if i < NSUB // 2:
                    ring(piece(src, p), 4, p, 2 * sg)
                ring(piece(src, p), 3, p, sg)
                to_partner(piece(src, p), 2, side)
        one = [arrived(1, 0), arrived(1, 1)]
        use("ring", two + one)
        use("pair", [from_partner(0, 0), from_partner(2, 0), from_partner(2, 1)])
        three = [arrived(3, 0), arrived(3, 1)]
        far = [arrived(4, 0)]
        use("pair", [from_partner(1, 0), from_partner(1, 1)])
        use("ring", three + far)
        for d, side in ((3, 0), (3, 1), (4, 0)):
            use("pair", [from_partner(d, side)])
        wait_sent(xg.at[dst, 0:7 + 2 * half], ag_s_sem)

    with jax.named_scope("stats"):
        ssq = jnp.zeros((rows, cw), F32)
        arrive(xg.at[0], x_sem)
        for k in range(FIRST, AHEAD):
            start_w(0, k, w_sem.at[k, 0], w_sem.at[k, 1])
        for k in range(nch):
            xf = xg[0, k].astype(F32)
            ssq = ssq + xf * xf
        set_inv_rms(jnp.sum(ssq, axis=1, keepdims=True))
        zero_acc()

    def l0_body(k, carry):
        b = lax.rem(k, RING)
        arrive(wqkv.at[k], w_sem.at[b, 0])
        arrive(wgu.at[k], w_sem.at[b, 1])
        do_chunk(0, k)

        @pl.when(k + AHEAD < nch)
        def _():
            nb = lax.rem(k + AHEAD, RING)
            start_w(0, k + AHEAD, w_sem.at[nb, 0], w_sem.at[nb, 1])

        @pl.when(k + AHEAD == nch)
        def _():
            start_kv(0)

        @pl.when(k + AHEAD == nch + 1)
        def _():
            start_all_od(0)
        return carry

    with jax.named_scope("kloop"):
        lax.fori_loop(0, nch, l0_body, 0)

    for l in range(layers):
        attention(l)
        with jax.named_scope(f"act{l}"):
            mlp_act()
        if l == 0:
            with jax.named_scope("barrier"):
                pl.semaphore_wait(barrier, tp - 1)
        with jax.named_scope(f"outproj{l}"):
            out_proj(l)
        if l + 1 < layers:
            for k in range(nch):
                start_w(l + 1, k, wl_sem.at[0], wl_sem.at[1])
            start_kv(l + 1)
            start_all_od(l + 1)
        with jax.named_scope(f"reduce{l}"):
            xn = reduce_own(l)
        xg[l + 1, me] = xn
        if l + 1 < layers:
            def use(kind, srcs, l=l):
                if kind == "early":
                    xf = xn.astype(F32)
                    sq = jnp.sum(xf * xf, axis=1, keepdims=True)
                    stats[l, me] = jnp.broadcast_to(sq, (rows, rows)).T[0:8, :]
                    for d in range(1, tp):
                        send(stats.at[l, me], stats.at[l, me], st_s_sem, st_r_sem, lax.rem(me + d, tp))
                    return
                if kind == "own":
                    zero_acc()
                    return
                if kind == "ring" and not use.ready:
                    use.ready = True
                    wait_recv(stats.at[l, 0:tp - 1], st_r_sem)
                    wait_sent(stats.at[l, 0:tp - 1], st_s_sem)
                    arrive(wqkv, wl_sem.at[0])
                    arrive(wgu, wl_sem.at[1])
                    tot = stats[l, 0]
                    for d in range(1, tp):
                        tot = tot + stats[l, d]
                    set_inv_rms(jnp.broadcast_to(tot[0:1, :], (rows, rows)).T[:, 0:1])
                    srcs = [me] + srcs
                for src in srcs:
                    do_chunk(l + 1, src)

            use.ready = False
            with jax.named_scope(f"gather{l}"):
                gather(l, use)
        else:
            def use_out(kind, srcs, l=l):
                for src in srcs:
                    pltpu.make_async_copy(xg.at[l + 1, src], out_hbm.at[:, pl.ds(pl.multiple_of(src * cw, cw), cw)], out_sem).start()

            with jax.named_scope(f"gather{l}"):
                gather(l, use_out)
            with jax.named_scope("outs"):
                arrive(xg.at[l + 1], out_sem)


def solution(mesh):
    tp = mesh.shape["tp"]
    arg_specs = (P("dp", None), P("dp"), P(), P(None, None, "tp"), P(None, None, "tp"), P(None, None, "tp"), P(None, "tp", None),
                 P(None, None, "tp"), P(None, None, "tp"), P(None, "tp", None), P(None, "dp", None, "tp", None), P(None, "dp", None, "tp", None))

    def per_device(x_in, lengths, norm_gain, w_q, w_k, w_v, w_o, w_gate, w_up, w_down, k_cache, v_cache):
        rows, width = x_in.shape
        layers, _, seq, hq, head = k_cache.shape
        ff = w_gate.shape[2]
        cw = width // tp
        chips = tp // 2
        assert w_q.shape[2] == cw == hq * head
        freq = (1.0 / (np.float32(ROPE_BASE) ** (np.arange(0, head, 2).astype(np.float32) / np.float32(head)))).astype(np.float32)
        freq = jnp.asarray(np.concatenate([freq, freq])[None, :])
        ffp = -(-(cw + ff) // 256) * 256 - cw
        kvr = rows * seq * hq
        ngrp = rows // 8
        m = hq * 8
        any_spec = pl.BlockSpec(memory_space=pl.ANY)
        vmem = pl.BlockSpec(memory_space=pltpu.VMEM)
        V = pltpu.VMEM
        D = pltpu.SemaphoreType.DMA
        scratch = [
            V((layers + 1, tp, rows, cw), BF16),
            V((tp, cw, 3 * cw), BF16),
            V((tp, 2, ff, cw), BF16),
            V((chips, cw + ffp, 2 * cw), BF16),
            V((kvr, head), BF16), V((kvr, head), BF16),
            V((layers, width), F32),
            V((rows, cw), F32),
            V((rows, rows), F32),
            V((rows, head), F32), V((rows, head), F32),
            V((rows, 3 * cw), F32),
            V((ff, rows), F32), V((ff, rows), F32),
            V((ffp, rows), F32),
            V((ngrp, hq, 8, head), F32), V((ngrp, hq, 8, head), F32), V((ngrp, hq, 8, head), F32),
            V((rows * hq, 8 * seq * hq), F32),
            V((rows * hq, 8 * seq * hq), BF16),
            V((rows, cw + ffp), BF16),
            V((rows, cw), F32),
            V((layers, chips, rows, cw), F32),
            V((layers, chips, rows, cw), F32),
            V((layers, chips, rows, cw), F32),
            V((layers, chips, rows, cw), BF16),
            V((layers, chips, rows, cw), BF16),
            V((layers, tp, 8, rows), F32),
            D(()), D((RING, 2)), D((2,)), D((2,)), D(()),
            D(()), D((chips,)), D(()), D((chips - 1,)), D(()), D(()),
            D(()), D((2 * NSUB + 5,)), D((chips,)), D(()),
        ]
        cfg = (tp, rows, width, ff, seq, head, hq, layers)
        return pl.pallas_call(
            functools.partial(decode_kernel, cfg),
            out_shape=jax.ShapeDtypeStruct((rows, width), BF16),
            in_specs=[any_spec, vmem, vmem, vmem] + [any_spec] * 9,
            out_specs=any_spec,
            scratch_shapes=scratch,
            compiler_params=pltpu.CompilerParams(collective_id=0, has_side_effects=True, vmem_limit_bytes=60 * 1024 * 1024),
        )(x_in, lengths.reshape(1, rows), freq, norm_gain, w_q, w_k, w_v, w_o, jnp.swapaxes(w_gate, 1, 2), jnp.swapaxes(w_up, 1, 2), w_down,
          k_cache.reshape(layers, kvr, head), v_cache.reshape(layers, kvr, head))

    return jax.shard_map(per_device, mesh=mesh, in_specs=arg_specs, out_specs=P("dp", None), check_vma=False)
```

```python
import functools

import numpy as np
import jax
import jax.numpy as jnp
from jax import lax
from jax.experimental import pallas as pl
from jax.experimental.pallas import tpu as pltpu
from jax.sharding import PartitionSpec as P

NORM_EPS = 1e-5
ROPE_BASE = 500000.0
F32 = jnp.float32
BF16 = jnp.bfloat16
NSUB = 2
LAG = 3
FIRST = 2
AHEAD = 7
RING = 8
VLIM = 54016


def decode_kernel(cfg, x_hbm, len_hbm, freq_hbm, gain_hbm, wq_hbm, wk_hbm, wv_hbm, wo_hbm, wg_hbm, wu_hbm, wd_hbm,
                  kc_hbm, vc_hbm, out_ref,
                  len_ref, freq_ref, gain_ref, xg, wqkv, wgu, wod, kbuf, vbuf, gain_s, rb, lenb, cosb, sinb, acc_qkv, acc_g, acc_u, ut,
                  qs, ks, vs, logit_s, prob_s, hbuf, attn_s, own_f, snd_f, rcv_f, shr_snd, shr_rcv, stats,
                  small_sem, x_sem, w_sem, wl_sem, kv_sem, od_sem, pair_s_sem, pair_r_sem, rs_s_sem, rs_r_sem, st_s_sem, st_r_sem,
                  ag_s_sem, ag_r_sem, pf_r_sem):
    tp, rows, width, ff, seq, head, hq, layers = cfg
    chips = tp // 2
    half = chips // 2
    pr = rows // NSUB
    cw = width // tp
    me = lax.axis_index("tp")
    z = me // 2
    c = lax.rem(me, 2)
    partner = z * 2 + (1 - c)
    scale = head ** -0.5
    nch = tp
    nqkv = 3 * cw
    grp = 8
    ngrp = rows // grp
    gcols = grp * seq * hq

    def ring_dev(off):
        return lax.rem(z + off + chips, chips) * 2 + c

    def x_copy(k):
        return pltpu.make_async_copy(x_hbm.at[:, pl.ds(k * cw, cw)], xg.at[0, k], x_sem)

    def start_w(l, k, qkv_sem, gu_sem):
        r = pl.ds(k * cw, cw)
        for i, w in enumerate((wq_hbm, wk_hbm, wv_hbm)):
            pltpu.make_async_copy(w.at[l, r, :], wqkv.at[k, :, i * cw:(i + 1) * cw], qkv_sem).start()
        for i, w in enumerate((wg_hbm, wu_hbm)):
            pltpu.make_async_copy(w.at[l, :, r], wgu.at[k, i], gu_sem).start()

    def start_kv(l):
        pltpu.make_async_copy(kc_hbm.at[l], kbuf, kv_sem.at[0]).start()
        pltpu.make_async_copy(vc_hbm.at[l], vbuf, kv_sem.at[1]).start()

    def start_od(l, j):
        cs = pl.ds(j * 2 * cw, 2 * cw)
        pltpu.make_async_copy(wo_hbm.at[l, :, cs], wod.at[j, 0:cw, :], od_sem).start()
        pltpu.make_async_copy(wd_hbm.at[l, :, cs], wod.at[j, cw:cw + ff, :], od_sem).start()

    def start_all_od(l):
        for i in range(chips):
            start_od(l, lax.rem(z + offs[i], chips))

    def arrive(ref, sem):
        pltpu.make_async_copy(ref, ref, sem).wait()

    def send(src, dst, s_sem, r_sem, dev):
        cp = pltpu.make_async_remote_copy(src_ref=src, dst_ref=dst, send_sem=s_sem, recv_sem=r_sem,
                                          device_id={"tp": dev}, device_id_type=pl.DeviceIdType.MESH)
        cp.start()

    def wait_remote(dst, sem):
        return pltpu.make_async_remote_copy(src_ref=dst, dst_ref=dst, send_sem=sem, recv_sem=sem,
                                            device_id={"tp": partner}, device_id_type=pl.DeviceIdType.MESH)

    def wait_recv(dst, sem):
        wait_remote(dst, sem).wait_recv()

    def wait_sent(src, sem):
        wait_remote(src, sem).wait_send()

    small = [pltpu.make_async_copy(src, dst, small_sem.at[i])
             for i, (src, dst) in enumerate(((len_hbm, len_ref), (freq_hbm, freq_ref), (gain_hbm, gain_ref)))]
    for cp in small:
        cp.start()
    offs = [half]
    for d in range(half - 1, 0, -1):
        offs += [d, chips - d]
    offs += [0]
    for k in range(nch):
        x_copy(k).start()
    for k in range(FIRST):
        start_w(0, k, w_sem.at[k, 0], w_sem.at[k, 1])

    scope_pre = jax.named_scope("pre")
    scope_pre.__enter__()
    barrier = pltpu.get_barrier_semaphore()
    for d in range(1, tp):
        pl.semaphore_signal(barrier, inc=1, device_id={"tp": lax.rem(me + d, tp)}, device_id_type=pl.DeviceIdType.MESH)

    pad = wod.shape[1] - cw - ff
    if pad:
        for j in range(chips):
            wod[j, cw + ff:, :] = jnp.zeros((pad, 2 * cw), BF16)
        ut[ff:, :] = jnp.zeros((pad, rows), F32)
    for cp in small:
        cp.wait()
    gain_s[...] = gain_ref[...].astype(F32)
    lenb[...] = jnp.broadcast_to(len_ref[...].astype(F32), (rows, rows)).T
    ang = lenb[...] * freq_ref[...]
    lane = lax.broadcasted_iota(jnp.int32, (rows, head), 1)
    cosb[...] = jnp.cos(ang)
    sn = jnp.sin(ang)
    sinb[...] = jnp.where(lane < head // 2, -sn, sn)
    scope_pre.__exit__(None, None, None)

    def set_inv_rms(ssq):
        inv = lax.rsqrt(ssq / width + NORM_EPS)
        rb[...] = jnp.broadcast_to(inv, rb.shape)

    def do_chunk(l, k):
        xk = xg[l, k].astype(F32)
        g = gain_s[l:l + 1, pl.ds(pl.multiple_of(k * cw, cw), cw)]
        a = (xk * rb[...] * g).astype(BF16)
        acc_qkv[...] += jnp.dot(a, wqkv[k], preferred_element_type=F32)
        nt = (((1,), (1,)), ((), ()))
        acc_g[...] += lax.dot_general(wgu[k, 0], a, nt, preferred_element_type=F32)
        acc_u[...] += lax.dot_general(wgu[k, 1], a, nt, preferred_element_type=F32)

    def rope(v):
        return (v * cosb[...] + pltpu.roll(v, head // 2, 1) * sinb[...]).astype(BF16).astype(F32)

    def zero_acc():
        acc_qkv[...] = jnp.zeros_like(acc_qkv)
        acc_g[...] = jnp.zeros_like(acc_g)
        acc_u[...] = jnp.zeros_like(acc_u)

    def attention(l):
        for h in range(hq):
            q = acc_qkv[:, h * head:(h + 1) * head].astype(BF16).astype(F32)
            k = acc_qkv[:, cw + h * head:cw + (h + 1) * head].astype(BF16).astype(F32)
            v = acc_qkv[:, 2 * cw + h * head:2 * cw + (h + 1) * head].astype(BF16).astype(F32)
            qs[:, h] = rope(q).reshape(ngrp, grp, head)
            ks[:, h] = rope(k).reshape(ngrp, grp, head)
            vs[:, h] = v.reshape(ngrp, grp, head)
        with jax.named_scope(f"kvwait{l}"):
            arrive(kbuf, kv_sem.at[0])
            arrive(vbuf, kv_sem.at[1])
        m = hq * grp
        for g in range(ngrp):
            q = qs[g].reshape(m, head).astype(BF16)
            kk = kbuf[g * gcols:(g + 1) * gcols, :]
            logit_s[g * m:(g + 1) * m, :] = lax.dot_general(q, kk, (((1,), (1,)), ((), ())), preferred_element_type=F32)
        col = lax.broadcasted_iota(jnp.int32, (m, gcols), 1)
        row = lax.broadcasted_iota(jnp.int32, (m, gcols), 0)
        same = ((col // (seq * hq)) == lax.rem(row, grp)) & (lax.rem(col, hq) == row // grp)
        key = jnp.where(same, lax.rem(col // hq, seq), 2 * seq).astype(F32)
        for g in range(ngrp):
            ln = lenb[g * grp:(g + 1) * grp, 0:1]
            ln = jnp.concatenate([ln] * hq, axis=0)
            lg = jnp.where(key < ln, logit_s[g * m:(g + 1) * m, :] * scale, -jnp.inf)
            qv = qs[g].reshape(m, head)
            kv = ks[g].reshape(m, head)
            vv = vs[g].reshape(m, head)
            sl = jnp.sum(qv * kv, axis=1, keepdims=True) * scale
            peak = jnp.maximum(jnp.max(lg, axis=1, keepdims=True), sl)
            w = jnp.exp(lg - peak)
            sw = jnp.exp(sl - peak)
            den = jnp.sum(w, axis=1, keepdims=True) + sw
            prob_s[g * m:(g + 1) * m, :] = (w / den).astype(BF16)
            sp = (sw / den).astype(BF16).astype(F32)
            vs[g] = (sp * vv).reshape(hq, grp, head)
        for g in range(ngrp):
            p = prob_s[g * m:(g + 1) * m, :]
            o = jnp.dot(p, vbuf[g * gcols:(g + 1) * gcols, :], preferred_element_type=F32)
            o = o + vs[g].reshape(m, head)
            for h in range(hq):
                attn_s[g * grp:(g + 1) * grp, h * head:(h + 1) * head] = o[h * grp:(h + 1) * grp]
        hbuf[:, 0:cw] = attn_s[...].astype(BF16)

    def mlp_act():
        gt = acc_g[...].astype(BF16).astype(F32)
        up = acc_u[...].astype(BF16).astype(F32)
        ut[0:ff, :] = gt * (1.0 / (1.0 + jnp.exp(-gt))) * up
        for i in range(ut.shape[0] // 128):
            hbuf[:, cw + i * 128:cw + (i + 1) * 128] = ut[i * 128:(i + 1) * 128, :].T.astype(BF16)

    def send_share(l, i, p):
        r = pl.ds(p * pr, pr)
        send(shr_snd.at[l, i, r, :], shr_rcv.at[l, i, r, :], rs_s_sem, rs_r_sem.at[p, i], ring_dev(offs[i]))

    def out_proj(l):
        arrive(wod.at[:, 0:cw + ff, :], od_sem)
        hv = hbuf[...]

        def finish(i):
            off = offs[i]
            wait_recv(rcv_f.at[l, i], pair_r_sem.at[i])
            s = own_f[l, i] + rcv_f[l, i]
            if off == 0:
                own_f[l, i] = s
            else:
                shr_snd[l, i] = s.astype(BF16)
                send_share(l, i, 0)

        for i in range(chips):
            j = lax.rem(z + offs[i], chips)
            p = jnp.dot(hv, wod[j], preferred_element_type=F32)
            lo, hi = p[:, :cw], p[:, cw:]
            own_f[l, i] = jnp.where(c == 0, lo, hi)
            snd_f[l, i] = jnp.where(c == 0, hi, lo)
            send(snd_f.at[l, i], rcv_f.at[l, i], pair_s_sem, pair_r_sem.at[i], partner)
            if i >= LAG:
                finish(i - LAG)
        for i in range(chips - LAG, chips):
            finish(i)
        for p in range(1, NSUB):
            for i in range(chips - 1):
                send_share(l, i, p)
        wait_sent(snd_f.at[l], pair_s_sem)

    def reduce_own(l, p):
        r = pl.ds(p * pr, pr)
        acc = xg[l, me, r, :].astype(F32) + own_f[l, chips - 1, r, :]
        for i in range(chips - 1):
            wait_recv(shr_rcv.at[l, i, r, :], rs_r_sem.at[p, i])
            acc = acc + shr_rcv[l, i, r, :].astype(F32)
        xg[l + 1, me, r, :] = acc.astype(BF16)

    def gather(l, use):
        dst = l + 1
        flip = 1 - 2 * c

        def piece(src, p):
            return xg.at[dst, src, pl.ds(p * pr, pr), :]

        def whole(src):
            return xg.at[dst, src]

        def slot(d, side):
            return 0 if d == 0 else (2 * half - 1 if d == half else 2 * d - 1 + side)

        def sem_of(d, side, p):
            return ag_r_sem.at[p * 2 + side] if d == 2 else ag_r_sem.at[2 * NSUB + (0 if d == half else (d // 2 + 1) * 2 - 1 + side)]

        def to_partner(ref, d, side):
            send(ref, ref, ag_s_sem, pf_r_sem.at[slot(d, side)], partner)

        def ring(ref, d, p, hops):
            send(ref, ref, ag_s_sem, sem_of(d, 0 if hops > 0 else 1, p), ring_dev(hops))

        def arrived(d, side):
            src = ring_dev(-d if side == 0 else d)
            wait_recv(whole(src), sem_of(d, side, 0))
            to_partner(whole(src), d, side)
            return src

        def from_partner(d, side):
            src = me + flip if d == 0 else ring_dev(-d if side == 0 else d) + flip
            wait_recv(whole(src), pf_r_sem.at[slot(d, side)])
            return src

        for p in range(NSUB):
            with jax.named_scope(f"reduce{l}p{p}"):
                reduce_own(l, p)
            ring(piece(me, p), 2, p, 2)
            ring(piece(me, p), 2, p, -2)
            if p == NSUB - 1:
                use("early", [])
            ring(piece(me, p), 1, p, 1)
            ring(piece(me, p), 1, p, -1)
            to_partner(piece(me, p), 0, 0)
        wait_sent(shr_snd.at[l, 0:chips - 1], rs_s_sem)
        use("own", [me])
        two = [ring_dev(-2), ring_dev(2)]
        for p in range(NSUB):
            for side in (0, 1):
                src = two[side]
                wait_recv(piece(src, p), sem_of(2, side, p))
                sg = 1 if side == 0 else -1
                if side == p // (NSUB // 2):
                    ring(piece(src, p), 4, p, 2 * sg)
                ring(piece(src, p), 3, p, sg)
                to_partner(piece(src, p), 2, side)
        one = [arrived(1, 0), arrived(1, 1)]
        use("ring", two + one)
        use("pair", [from_partner(0, 0), from_partner(2, 0), from_partner(2, 1)])
        three = [arrived(3, 0), arrived(3, 1)]
        far = [arrived(4, 0)]
        use("pair", [from_partner(1, 0), from_partner(1, 1)])
        use("ring", three + far)
        for d, side in ((3, 0), (3, 1), (4, 0)):
            use("pair", [from_partner(d, side)])
        wait_sent(xg.at[dst, 0:7 + 2 * half], ag_s_sem)

    with jax.named_scope("stats"):
        ssq = jnp.zeros((rows, cw), F32)
        arrive(xg.at[0], x_sem)
        for k in range(FIRST, AHEAD):
            start_w(0, k, w_sem.at[k, 0], w_sem.at[k, 1])
        for k in range(nch):
            xf = xg[0, k].astype(F32)
            ssq = ssq + xf * xf
        set_inv_rms(jnp.sum(ssq, axis=1, keepdims=True))
        zero_acc()

    def l0_body(k, carry):
        b = lax.rem(k, RING)
        arrive(wqkv.at[k], w_sem.at[b, 0])
        arrive(wgu.at[k], w_sem.at[b, 1])
        do_chunk(0, k)

        @pl.when(k + AHEAD < nch)
        def _():
            nb = lax.rem(k + AHEAD, RING)
            start_w(0, k + AHEAD, w_sem.at[nb, 0], w_sem.at[nb, 1])

        @pl.when(k + AHEAD == nch)
        def _():
            start_kv(0)

        @pl.when(k + AHEAD == nch + 1)
        def _():
            start_all_od(0)
        return carry

    with jax.named_scope("kloop"):
        lax.fori_loop(0, nch, l0_body, 0)

    for l in range(layers):
        attention(l)
        with jax.named_scope(f"act{l}"):
            mlp_act()
        if l == 0:
            with jax.named_scope("barrier"):
                pl.semaphore_wait(barrier, tp - 1)
        with jax.named_scope(f"outproj{l}"):
            out_proj(l)
        if l + 1 < layers:
            for k in range(nch):
                start_w(l + 1, k, wl_sem.at[0], wl_sem.at[1])
            start_kv(l + 1)
            start_all_od(l + 1)
        if l + 1 < layers:
            def use(kind, srcs, l=l):
                if kind == "early":
                    xf = xg[l + 1, me].astype(F32)
                    sq = jnp.sum(xf * xf, axis=1, keepdims=True)
                    stats[l, me] = jnp.broadcast_to(sq, (rows, rows)).T[0:8, :]
                    for d in range(1, tp):
                        send(stats.at[l, me], stats.at[l, me], st_s_sem, st_r_sem, lax.rem(me + d, tp))
                    return
                if kind == "own":
                    zero_acc()
                    return
                if kind == "ring" and not use.ready:
                    use.ready = True
                    wait_recv(stats.at[l, 0:tp - 1], st_r_sem)
                    wait_sent(stats.at[l, 0:tp - 1], st_s_sem)
                    arrive(wqkv, wl_sem.at[0])
                    arrive(wgu, wl_sem.at[1])
                    tot = stats[l, 0]
                    for d in range(1, tp):
                        tot = tot + stats[l, d]
                    set_inv_rms(jnp.broadcast_to(tot[0:1, :], (rows, rows)).T[:, 0:1])
                    srcs = [me] + srcs
                for src in srcs:
                    do_chunk(l + 1, src)

            use.ready = False
            with jax.named_scope(f"gather{l}"):
                gather(l, use)
        else:
            def use_out(kind, srcs, l=l):
                for src in srcs:
                    out_ref[:, pl.ds(pl.multiple_of(src * cw, cw), cw)] = xg[l + 1, src]

            with jax.named_scope(f"gather{l}"):
                gather(l, use_out)


def solution(mesh):
    tp = mesh.shape["tp"]
    arg_specs = (P("dp", None), P("dp"), P(), P(None, None, "tp"), P(None, None, "tp"), P(None, None, "tp"), P(None, "tp", None),
                 P(None, None, "tp"), P(None, None, "tp"), P(None, "tp", None), P(None, "dp", None, "tp", None), P(None, "dp", None, "tp", None))

    def per_device(x_in, lengths, norm_gain, w_q, w_k, w_v, w_o, w_gate, w_up, w_down, k_cache, v_cache):
        rows, width = x_in.shape
        layers, _, seq, hq, head = k_cache.shape
        ff = w_gate.shape[2]
        cw = width // tp
        chips = tp // 2
        assert w_q.shape[2] == cw == hq * head
        freq = (1.0 / (np.float32(ROPE_BASE) ** (np.arange(0, head, 2).astype(np.float32) / np.float32(head)))).astype(np.float32)
        freq = jnp.asarray(np.concatenate([freq, freq])[None, :])
        ffp = -(-(cw + ff) // 256) * 256 - cw
        kvr = rows * seq * hq
        ngrp = rows // 8
        m = hq * 8
        pin = lambda v: pltpu.with_memory_space_constraint(v, pltpu.HBM)
        hbm = pl.BlockSpec(memory_space=pltpu.HBM)
        any_spec = pl.BlockSpec(memory_space=pl.ANY)
        vmem = pl.BlockSpec(memory_space=pltpu.VMEM)
        V = pltpu.VMEM
        D = pltpu.SemaphoreType.DMA
        scratch = [
            V((1, rows), jnp.int32), V((1, head), F32), V((layers, width), BF16),
            V((layers + 1, tp, rows, cw), BF16),
            V((tp, cw, 3 * cw), BF16),
            V((tp, 2, ff, cw), BF16),
            V((chips, cw + ffp, 2 * cw), BF16),
            V((kvr, head), BF16), V((kvr, head), BF16),
            V((layers, width), F32),
            V((rows, cw), F32),
            V((rows, rows), F32),
            V((rows, head), F32), V((rows, head), F32),
            V((rows, 3 * cw), F32),
            V((ff, rows), F32), V((ff, rows), F32),
            V((ffp, rows), F32),
            V((ngrp, hq, 8, head), F32), V((ngrp, hq, 8, head), F32), V((ngrp, hq, 8, head), F32),
            V((rows * hq, 8 * seq * hq), F32),
            V((rows * hq, 8 * seq * hq), BF16),
            V((rows, cw + ffp), BF16),
            V((rows, cw), F32),
            V((layers, chips, rows, cw), F32),
            V((layers, chips, rows, cw), F32),
            V((layers, chips, rows, cw), F32),
            V((layers, chips, rows, cw), BF16),
            V((layers, chips, rows, cw), BF16),
            V((layers, tp, 8, rows), F32),
            D((3,)), D(()), D((RING, 2)), D((2,)), D((2,)), D(()),
            D(()), D((chips,)), D(()), D((NSUB, chips - 1)), D(()), D(()),
            D(()), D((2 * NSUB + 5,)), D((chips,)),
        ]
        cfg = (tp, rows, width, ff, seq, head, hq, layers)
        return pl.pallas_call(
            functools.partial(decode_kernel, cfg),
            out_shape=jax.ShapeDtypeStruct((rows, width), BF16),
            in_specs=[any_spec, hbm, hbm, hbm] + [any_spec] * 9,
            out_specs=vmem,
            scratch_shapes=scratch,
            compiler_params=pltpu.CompilerParams(collective_id=0, has_side_effects=True, vmem_limit_bytes=VLIM * 1024),
        )(x_in, pin(lengths.reshape(1, rows)), pin(freq), pin(norm_gain), w_q, w_k, w_v, w_o, jnp.swapaxes(w_gate, 1, 2), jnp.swapaxes(w_up, 1, 2), w_down,
          k_cache.reshape(layers, kvr, head), v_cache.reshape(layers, kvr, head))

    return jax.shard_map(per_device, mesh=mesh, in_specs=arg_specs, out_specs=P("dp", None), check_vma=False)
```

```python
import functools

import numpy as np
import jax
import jax.numpy as jnp
from jax import lax
from jax.experimental import pallas as pl
from jax.experimental.pallas import tpu as pltpu
from jax.sharding import PartitionSpec as P

NORM_EPS = 1e-5
ROPE_BASE = 500000.0
F32 = jnp.float32
BF16 = jnp.bfloat16
NSUB = 2
LAG = 3
FIRST = 3
AHEAD = 8
RING = 8
UNROLL = 2
WIDE = 2
KV_AT = 3
VLIM = 54016


def decode_kernel(cfg, x_hbm, len_hbm, freq_hbm, gain_hbm, wq_hbm, wk_hbm, wv_hbm, wo_hbm, wg_hbm, wu_hbm, wd_hbm,
                  kc_hbm, vc_hbm, out_ref,
                  len_ref, freq_ref, gain_ref, xg, wqkv, wgu, wod, kbuf, vbuf, gain_s, rb, lenb, cosb, sinb, acc_qkv, acc_g, acc_u, ut,
                  qs, ks, vs, logit_s, prob_s, hbuf, attn_s, own_f, snd_f, rcv_f, shr_snd, shr_rcv, stats,
                  small_sem, x_sem, w_sem, wl_sem, kv_sem, od_sem, pair_s_sem, pair_r_sem, rs_s_sem, rs_r_sem, st_s_sem, st_r_sem,
                  ag_s_sem, ag_r_sem, pf_r_sem):
    tp, rows, width, ff, seq, head, hq, layers = cfg
    chips = tp // 2
    half = chips // 2
    pr = rows // NSUB
    cw = width // tp
    me = lax.axis_index("tp")
    z = me // 2
    c = lax.rem(me, 2)
    partner = z * 2 + (1 - c)
    scale = head ** -0.5
    nch = tp
    nqkv = 3 * cw
    grp = 8
    ngrp = rows // grp
    gcols = grp * seq * hq

    def ring_dev(off):
        return lax.rem(z + off + chips, chips) * 2 + c

    def x_copy(k):
        return pltpu.make_async_copy(x_hbm.at[:, pl.ds(k * cw, cw)], xg.at[0, k], x_sem)

    def start_w(l, k, qkv_sem, gu_sem):
        r = pl.ds(k * cw, cw)
        for i, w in enumerate((wq_hbm, wk_hbm, wv_hbm)):
            pltpu.make_async_copy(w.at[l, r, :], wqkv.at[k, :, i * cw:(i + 1) * cw], qkv_sem).start()
        for i, w in enumerate((wg_hbm, wu_hbm)):
            pltpu.make_async_copy(w.at[l, :, r], wgu.at[k, i], gu_sem).start()

    def start_kv(l):
        pltpu.make_async_copy(kc_hbm.at[l], kbuf, kv_sem.at[0]).start()
        pltpu.make_async_copy(vc_hbm.at[l], vbuf, kv_sem.at[1]).start()

    def start_od(l, i):
        j = lax.rem(z + offs[i], chips)
        cs = pl.ds(j * 2 * cw, 2 * cw)
        pltpu.make_async_copy(wo_hbm.at[l, :, cs], wod.at[j, 0:cw, :], od_sem.at[i]).start()
        pltpu.make_async_copy(wd_hbm.at[l, :, cs], wod.at[j, cw:cw + ff, :], od_sem.at[i]).start()

    def arrive(ref, sem):
        pltpu.make_async_copy(ref, ref, sem).wait()

    def send(src, dst, s_sem, r_sem, dev):
        cp = pltpu.make_async_remote_copy(src_ref=src, dst_ref=dst, send_sem=s_sem, recv_sem=r_sem,
                                          device_id={"tp": dev}, device_id_type=pl.DeviceIdType.MESH)
        cp.start()

    def wait_remote(dst, sem):
        return pltpu.make_async_remote_copy(src_ref=dst, dst_ref=dst, send_sem=sem, recv_sem=sem,
                                            device_id={"tp": partner}, device_id_type=pl.DeviceIdType.MESH)

    def wait_recv(dst, sem):
        wait_remote(dst, sem).wait_recv()

    def wait_sent(src, sem):
        wait_remote(src, sem).wait_send()

    small = [pltpu.make_async_copy(src, dst, small_sem.at[i])
             for i, (src, dst) in enumerate(((len_hbm, len_ref), (freq_hbm, freq_ref), (gain_hbm, gain_ref)))]
    for cp in small:
        cp.start()
    offs = [half]
    for d in range(half - 1, 0, -1):
        offs += [d, chips - d]
    offs += [0]
    for k in range(nch):
        x_copy(k).start()
    for k in range(FIRST):
        start_w(0, k, w_sem.at[k, 0], w_sem.at[k, 1])

    scope_pre = jax.named_scope("pre")
    scope_pre.__enter__()
    barrier = pltpu.get_barrier_semaphore()
    for d in range(1, tp):
        pl.semaphore_signal(barrier, inc=1, device_id={"tp": lax.rem(me + d, tp)}, device_id_type=pl.DeviceIdType.MESH)

    pad = wod.shape[1] - cw - ff
    if pad:
        for j in range(chips):
            wod[j, cw + ff:, :] = jnp.zeros((pad, 2 * cw), BF16)
        ut[ff:, :] = jnp.zeros((pad, rows), F32)
    for cp in small:
        cp.wait()
    for k in range(FIRST, AHEAD):
        start_w(0, k, w_sem.at[k, 0], w_sem.at[k, 1])
    gain_s[...] = gain_ref[...].astype(F32)
    lenb[...] = jnp.broadcast_to(len_ref[...].astype(F32), (rows, rows)).T
    ang = lenb[...] * freq_ref[...]
    lane = lax.broadcasted_iota(jnp.int32, (rows, head), 1)
    cosb[...] = jnp.cos(ang)
    sn = jnp.sin(ang)
    sinb[...] = jnp.where(lane < head // 2, -sn, sn)
    scope_pre.__exit__(None, None, None)

    def set_inv_rms(ssq):
        inv = lax.rsqrt(ssq / width + NORM_EPS)
        rb[...] = jnp.broadcast_to(inv, rb.shape)

    def do_chunks(l, ks):
        nt = (((1,), (1,)), ((), ()))

        def join(parts, axis):
            return parts[0] if len(parts) == 1 else jnp.concatenate(parts, axis=axis)

        a = []
        for k in ks:
            g = gain_s[l:l + 1, pl.ds(pl.multiple_of(k * cw, cw), cw)]
            a.append((xg[l, k].astype(F32) * rb[...] * g).astype(BF16))
        a = join(a, 1)
        acc_qkv[...] += jnp.dot(a, join([wqkv[k] for k in ks], 0), preferred_element_type=F32)
        acc_g[...] += lax.dot_general(join([wgu[k, 0] for k in ks], 1), a, nt, preferred_element_type=F32)
        acc_u[...] += lax.dot_general(join([wgu[k, 1] for k in ks], 1), a, nt, preferred_element_type=F32)

    def rope(v):
        return (v * cosb[...] + pltpu.roll(v, head // 2, 1) * sinb[...]).astype(BF16).astype(F32)

    def zero_acc():
        acc_qkv[...] = jnp.zeros_like(acc_qkv)
        acc_g[...] = jnp.zeros_like(acc_g)
        acc_u[...] = jnp.zeros_like(acc_u)

    def attention(l):
        for h in range(hq):
            q = acc_qkv[:, h * head:(h + 1) * head].astype(BF16).astype(F32)
            k = acc_qkv[:, cw + h * head:cw + (h + 1) * head].astype(BF16).astype(F32)
            v = acc_qkv[:, 2 * cw + h * head:2 * cw + (h + 1) * head].astype(BF16).astype(F32)
            qs[:, h] = rope(q).reshape(ngrp, grp, head)
            ks[:, h] = rope(k).reshape(ngrp, grp, head)
            vs[:, h] = v.reshape(ngrp, grp, head)
        with jax.named_scope(f"kvwait{l}"):
            arrive(kbuf, kv_sem.at[0])
            arrive(vbuf, kv_sem.at[1])
        m = hq * grp
        for g in range(ngrp):
            q = qs[g].reshape(m, head).astype(BF16)
            kk = kbuf[g * gcols:(g + 1) * gcols, :]
            logit_s[g * m:(g + 1) * m, :] = lax.dot_general(q, kk, (((1,), (1,)), ((), ())), preferred_element_type=F32)
        col = lax.broadcasted_iota(jnp.int32, (m, gcols), 1)
        row = lax.broadcasted_iota(jnp.int32, (m, gcols), 0)
        same = ((col // (seq * hq)) == lax.rem(row, grp)) & (lax.rem(col, hq) == row // grp)
        key = jnp.where(same, lax.rem(col // hq, seq), 2 * seq).astype(F32)
        for g in range(ngrp):
            ln = lenb[g * grp:(g + 1) * grp, 0:1]
            ln = jnp.concatenate([ln] * hq, axis=0)
            lg = jnp.where(key < ln, logit_s[g * m:(g + 1) * m, :] * scale, -jnp.inf)
            qv = qs[g].reshape(m, head)
            kv = ks[g].reshape(m, head)
            vv = vs[g].reshape(m, head)
            sl = jnp.sum(qv * kv, axis=1, keepdims=True) * scale
            peak = jnp.maximum(jnp.max(lg, axis=1, keepdims=True), sl)
            w = jnp.exp(lg - peak)
            sw = jnp.exp(sl - peak)
            den = jnp.sum(w, axis=1, keepdims=True) + sw
            prob_s[g * m:(g + 1) * m, :] = (w / den).astype(BF16)
            sp = (sw / den).astype(BF16).astype(F32)
            vs[g] = (sp * vv).reshape(hq, grp, head)
        for g in range(ngrp):
            p = prob_s[g * m:(g + 1) * m, :]
            o = jnp.dot(p, vbuf[g * gcols:(g + 1) * gcols, :], preferred_element_type=F32)
            o = o + vs[g].reshape(m, head)
            for h in range(hq):
                attn_s[g * grp:(g + 1) * grp, h * head:(h + 1) * head] = o[h * grp:(h + 1) * grp]
        hbuf[:, 0:cw] = attn_s[...].astype(BF16)

    def mlp_act():
        gt = acc_g[...].astype(BF16).astype(F32)
        up = acc_u[...].astype(BF16).astype(F32)
        ut[0:ff, :] = gt * (1.0 / (1.0 + jnp.exp(-gt))) * up
        for i in range(ut.shape[0] // 128):
            hbuf[:, cw + i * 128:cw + (i + 1) * 128] = ut[i * 128:(i + 1) * 128, :].T.astype(BF16)

    def send_share(l, i, p):
        r = pl.ds(p * pr, pr)
        send(shr_snd.at[l, i, r, :], shr_rcv.at[l, i, r, :], rs_s_sem, rs_r_sem.at[p, i], ring_dev(offs[i]))

    def out_proj(l):
        hv = hbuf[...]

        def finish(i):
            off = offs[i]
            wait_recv(rcv_f.at[l, i], pair_r_sem.at[i])
            s = own_f[l, i] + rcv_f[l, i]
            if off == 0:
                own_f[l, i] = s
            else:
                shr_snd[l, i] = s.astype(BF16)
                send_share(l, i, 0)

        for i in range(chips):
            j = lax.rem(z + offs[i], chips)
            arrive(wod.at[j, 0:cw + ff, :], od_sem.at[i])
            p = jnp.dot(hv, wod[j], preferred_element_type=F32)
            lo, hi = p[:, :cw], p[:, cw:]
            own_f[l, i] = jnp.where(c == 0, lo, hi)
            snd_f[l, i] = jnp.where(c == 0, hi, lo)
            send(snd_f.at[l, i], rcv_f.at[l, i], pair_s_sem, pair_r_sem.at[i], partner)
            if i >= LAG:
                finish(i - LAG)
        for i in range(chips - LAG, chips):
            finish(i)
        for p in range(1, NSUB):
            for i in range(chips - 1):
                send_share(l, i, p)
        wait_sent(snd_f.at[l], pair_s_sem)

    def reduce_own(l, p):
        r = pl.ds(p * pr, pr)
        acc = xg[l, me, r, :].astype(F32) + own_f[l, chips - 1, r, :]
        for i in range(chips - 1):
            wait_recv(shr_rcv.at[l, i, r, :], rs_r_sem.at[p, i])
            acc = acc + shr_rcv[l, i, r, :].astype(F32)
        xg[l + 1, me, r, :] = acc.astype(BF16)

    def gather(l, use):
        dst = l + 1
        flip = 1 - 2 * c

        def piece(src, p):
            return xg.at[dst, src, pl.ds(p * pr, pr), :]

        def whole(src):
            return xg.at[dst, src]

        def slot(d, side):
            return 0 if d == 0 else (2 * half - 1 if d == half else 2 * d - 1 + side)

        def sem_of(d, side, p):
            return ag_r_sem.at[p * 2 + side] if d == 2 else ag_r_sem.at[2 * NSUB + (0 if d == half else (d // 2 + 1) * 2 - 1 + side)]

        def to_partner(ref, d, side):
            send(ref, ref, ag_s_sem, pf_r_sem.at[slot(d, side)], partner)

        def ring(ref, d, p, hops):
            send(ref, ref, ag_s_sem, sem_of(d, 0 if hops > 0 else 1, p), ring_dev(hops))

        def arrived(d, side):
            src = ring_dev(-d if side == 0 else d)
            wait_recv(whole(src), sem_of(d, side, 0))
            to_partner(whole(src), d, side)
            return src

        def from_partner(d, side):
            src = me + flip if d == 0 else ring_dev(-d if side == 0 else d) + flip
            wait_recv(whole(src), pf_r_sem.at[slot(d, side)])
            return src

        for p in range(NSUB):
            with jax.named_scope(f"reduce{l}p{p}"):
                reduce_own(l, p)
            ring(piece(me, p), 2, p, 2)
            ring(piece(me, p), 2, p, -2)
            if p == NSUB - 1:
                use("early", [])
            ring(piece(me, p), 1, p, 1)
            ring(piece(me, p), 1, p, -1)
            to_partner(piece(me, p), 0, 0)
        wait_sent(shr_snd.at[l, 0:chips - 1], rs_s_sem)
        use("own", [me])
        two = [ring_dev(-2), ring_dev(2)]
        for p in range(NSUB):
            for side in (0, 1):
                src = two[side]
                wait_recv(piece(src, p), sem_of(2, side, p))
                sg = 1 if side == 0 else -1
                if side == p // (NSUB // 2):
                    ring(piece(src, p), 4, p, 2 * sg)
                ring(piece(src, p), 3, p, sg)
                to_partner(piece(src, p), 2, side)
        one = [arrived(1, 0), arrived(1, 1)]
        use("ring", two + one)
        use("pair", [from_partner(0, 0), from_partner(2, 0), from_partner(2, 1)])
        three = [arrived(3, 0), arrived(3, 1)]
        far = [arrived(4, 0)]
        use("pair", [from_partner(1, 0), from_partner(1, 1)])
        use("ring", three + far)
        for d, side in ((3, 0), (3, 1), (4, 0)):
            use("pair", [from_partner(d, side)])
        wait_sent(xg.at[dst, 0:7 + 2 * half], ag_s_sem)

    with jax.named_scope("stats"):
        ssq = jnp.zeros((rows, cw), F32)
        arrive(xg.at[0], x_sem)
        for k in range(nch):
            xf = xg[0, k].astype(F32)
            ssq = ssq + xf * xf
        set_inv_rms(jnp.sum(ssq, axis=1, keepdims=True))
        zero_acc()

    def l0_body(i, carry):
        ks = [i * UNROLL + u for u in range(UNROLL)]
        for k in ks:
            b = lax.rem(k, RING)
            arrive(wqkv.at[k], w_sem.at[b, 0])
            arrive(wgu.at[k], w_sem.at[b, 1])
        for k in ks:
            @pl.when(k + AHEAD < nch)
            def _(k=k):
                nb = lax.rem(k + AHEAD, RING)
                start_w(0, k + AHEAD, w_sem.at[nb, 0], w_sem.at[nb, 1])

        @pl.when(i == KV_AT)
        def _():
            start_kv(0)
        for b in range(chips // 2):
            @pl.when(i == (nch - AHEAD) // UNROLL + b)
            def _(b=b):
                start_od(0, 2 * b)
                start_od(0, 2 * b + 1)
        do_chunks(0, ks)
        return carry

    with jax.named_scope("kloop"):
        lax.fori_loop(0, nch // UNROLL, l0_body, 0)

    for l in range(layers):
        attention(l)
        with jax.named_scope(f"act{l}"):
            mlp_act()
        if l == 0:
            with jax.named_scope("barrier"):
                pl.semaphore_wait(barrier, tp - 1)
        with jax.named_scope(f"outproj{l}"):
            out_proj(l)
        if l + 1 < layers:
            for k in range(nch):
                start_w(l + 1, k, wl_sem.at[0], wl_sem.at[1])
            start_kv(l + 1)
            for i in range(chips):
                start_od(l + 1, i)
        if l + 1 < layers:
            def use(kind, srcs, l=l):
                if kind == "early":
                    xf = xg[l + 1, me].astype(F32)
                    sq = jnp.sum(xf * xf, axis=1, keepdims=True)
                    stats[l, me] = jnp.broadcast_to(sq, (rows, rows)).T[0:1, :]
                    for d in range(1, tp):
                        send(stats.at[l, me], stats.at[l, me], st_s_sem, st_r_sem, lax.rem(me + d, tp))
                    return
                if kind == "own":
                    zero_acc()
                    return
                if kind == "ring" and not use.ready:
                    use.ready = True
                    wait_recv(stats.at[l, 0:tp - 1], st_r_sem)
                    wait_sent(stats.at[l, 0:tp - 1], st_s_sem)
                    arrive(wqkv, wl_sem.at[0])
                    arrive(wgu, wl_sem.at[1])
                    tot = stats[l, 0]
                    for d in range(1, tp):
                        tot = tot + stats[l, d]
                    set_inv_rms(jnp.broadcast_to(tot, (rows, rows)).T[:, 0:1])
                    srcs = [me] + srcs
                for n in range(0, len(srcs), WIDE):
                    do_chunks(l + 1, srcs[n:n + WIDE])

            use.ready = False
            with jax.named_scope(f"gather{l}"):
                gather(l, use)
        else:
            def use_out(kind, srcs, l=l):
                for src in srcs:
                    out_ref[:, pl.ds(pl.multiple_of(src * cw, cw), cw)] = xg[l + 1, src]

            with jax.named_scope(f"gather{l}"):
                gather(l, use_out)


def solution(mesh):
    tp = mesh.shape["tp"]
    arg_specs = (P("dp", None), P("dp"), P(), P(None, None, "tp"), P(None, None, "tp"), P(None, None, "tp"), P(None, "tp", None),
                 P(None, None, "tp"), P(None, None, "tp"), P(None, "tp", None), P(None, "dp", None, "tp", None), P(None, "dp", None, "tp", None))

    def per_device(x_in, lengths, norm_gain, w_q, w_k, w_v, w_o, w_gate, w_up, w_down, k_cache, v_cache):
        rows, width = x_in.shape
        layers, _, seq, hq, head = k_cache.shape
        ff = w_gate.shape[2]
        cw = width // tp
        chips = tp // 2
        assert w_q.shape[2] == cw == hq * head
        freq = (1.0 / (np.float32(ROPE_BASE) ** (np.arange(0, head, 2).astype(np.float32) / np.float32(head)))).astype(np.float32)
        freq = jnp.asarray(np.concatenate([freq, freq])[None, :])
        ffp = -(-(cw + ff) // 256) * 256 - cw
        kvr = rows * seq * hq
        ngrp = rows // 8
        m = hq * 8
        pin = lambda v: pltpu.with_memory_space_constraint(v, pltpu.HBM)
        hbm = pl.BlockSpec(memory_space=pltpu.HBM)
        any_spec = pl.BlockSpec(memory_space=pl.ANY)
        vmem = pl.BlockSpec(memory_space=pltpu.VMEM)
        V = pltpu.VMEM
        D = pltpu.SemaphoreType.DMA
        scratch = [
            V((1, rows), jnp.int32), V((1, head), F32), V((layers, width), BF16),
            V((layers + 1, tp, rows, cw), BF16),
            V((tp, cw, 3 * cw), BF16),
            V((tp, 2, ff, cw), BF16),
            V((chips, cw + ffp, 2 * cw), BF16),
            V((kvr, head), BF16), V((kvr, head), BF16),
            V((layers, width), F32),
            V((rows, cw), F32),
            V((rows, rows), F32),
            V((rows, head), F32), V((rows, head), F32),
            V((rows, 3 * cw), F32),
            V((ff, rows), F32), V((ff, rows), F32),
            V((ffp, rows), F32),
            V((ngrp, hq, 8, head), F32), V((ngrp, hq, 8, head), F32), V((ngrp, hq, 8, head), F32),
            V((rows * hq, 8 * seq * hq), F32),
            V((rows * hq, 8 * seq * hq), BF16),
            V((rows, cw + ffp), BF16),
            V((rows, cw), F32),
            V((layers, chips, rows, cw), F32),
            V((layers, chips, rows, cw), F32),
            V((layers, chips, rows, cw), F32),
            V((layers, chips, rows, cw), BF16),
            V((layers, chips, rows, cw), BF16),
            V((layers, tp, 1, rows), F32),
            D((3,)), D(()), D((RING, 2)), D((2,)), D((2,)), D((chips,)),
            D(()), D((chips,)), D(()), D((NSUB, chips - 1)), D(()), D(()),
            D(()), D((2 * NSUB + 5,)), D((chips,)),
        ]
        cfg = (tp, rows, width, ff, seq, head, hq, layers)
        return pl.pallas_call(
            functools.partial(decode_kernel, cfg),
            out_shape=jax.ShapeDtypeStruct((rows, width), BF16),
            in_specs=[any_spec, hbm, hbm, hbm] + [any_spec] * 9,
            out_specs=vmem,
            scratch_shapes=scratch,
            compiler_params=pltpu.CompilerParams(collective_id=0, has_side_effects=True, vmem_limit_bytes=VLIM * 1024),
        )(x_in, pin(lengths.reshape(1, rows)), pin(freq), pin(norm_gain), w_q, w_k, w_v, w_o, jnp.swapaxes(w_gate, 1, 2), jnp.swapaxes(w_up, 1, 2), w_down,
          k_cache.reshape(layers, kvr, head), v_cache.reshape(layers, kvr, head))

    return jax.shard_map(per_device, mesh=mesh, in_specs=arg_specs, out_specs=P("dp", None), check_vma=False)
```

```python
import functools

import numpy as np
import jax
import jax.numpy as jnp
from jax import lax
from jax.experimental import pallas as pl
from jax.experimental.pallas import tpu as pltpu
from jax.sharding import PartitionSpec as P

NORM_EPS = 1e-5
ROPE_BASE = 500000.0
F32 = jnp.float32
BF16 = jnp.bfloat16
NSUB = 2
LAG = 3
FIRST = 3
AHEAD = 8
RING = 8
UNROLL = 2
WIDE = 2
KV_AT = 3
VLIM = 54016


def decode_kernel(cfg, x_hbm, len_hbm, freq_hbm, gain_hbm, wq_hbm, wk_hbm, wv_hbm, wo_hbm, wg_hbm, wu_hbm, wd_hbm,
                  kc_hbm, vc_hbm, out_ref,
                  len_ref, freq_ref, gain_ref, xg, wqkv, wgu, wod, kbuf, vbuf, gain_s, rb, lenb, cosb, sinb, acc_qkv, acc_g, acc_u, ut,
                  qs, ks, vs, logit_s, prob_s, hbuf, attn_s, own_f, snd_f, rcv_f, shr_snd, shr_rcv, stats,
                  small_sem, x_sem, w_sem, wl_sem, kv_sem, od_sem, pair_s_sem, pair_r_sem, rs_s_sem, rs_r_sem, st_s_sem, st_r_sem,
                  ag_s_sem, ag_r_sem, pf_r_sem):
    tp, rows, width, ff, seq, head, hq, layers = cfg
    chips = tp // 2
    half = chips // 2
    pr = rows // NSUB
    cw = width // tp
    me = lax.axis_index("tp")
    z = me // 2
    c = lax.rem(me, 2)
    partner = z * 2 + (1 - c)
    scale = head ** -0.5
    nch = tp
    nqkv = 3 * cw
    grp = 8
    ngrp = rows // grp
    gcols = grp * seq * hq

    def ring_dev(off):
        return lax.rem(z + off + chips, chips) * 2 + c

    def x_copy(k):
        return pltpu.make_async_copy(x_hbm.at[:, pl.ds(k * cw, cw)], xg.at[0, k], x_sem)

    def start_w(l, k, qkv_sem, gu_sem):
        r = pl.ds(k * cw, cw)
        for i, w in enumerate((wq_hbm, wk_hbm, wv_hbm)):
            pltpu.make_async_copy(w.at[l, r, :], wqkv.at[k, :, i * cw:(i + 1) * cw], qkv_sem).start()
        for i, w in enumerate((wg_hbm, wu_hbm)):
            pltpu.make_async_copy(w.at[l, :, r], wgu.at[k, i], gu_sem).start()

    def start_kv(l):
        pltpu.make_async_copy(kc_hbm.at[l], kbuf, kv_sem.at[0]).start()
        pltpu.make_async_copy(vc_hbm.at[l], vbuf, kv_sem.at[1]).start()

    def start_od(l, i):
        j = lax.rem(z + offs[i], chips)
        cs = pl.ds(j * 2 * cw, 2 * cw)
        pltpu.make_async_copy(wo_hbm.at[l, :, cs], wod.at[j, 0:cw, :], od_sem.at[i]).start()
        pltpu.make_async_copy(wd_hbm.at[l, :, cs], wod.at[j, cw:cw + ff, :], od_sem.at[i]).start()

    def arrive(ref, sem):
        pltpu.make_async_copy(ref, ref, sem).wait()

    def send(src, dst, s_sem, r_sem, dev):
        cp = pltpu.make_async_remote_copy(src_ref=src, dst_ref=dst, send_sem=s_sem, recv_sem=r_sem,
                                          device_id={"tp": dev}, device_id_type=pl.DeviceIdType.MESH)
        cp.start()

    def wait_remote(dst, sem):
        return pltpu.make_async_remote_copy(src_ref=dst, dst_ref=dst, send_sem=sem, recv_sem=sem,
                                            device_id={"tp": partner}, device_id_type=pl.DeviceIdType.MESH)

    def wait_recv(dst, sem):
        wait_remote(dst, sem).wait_recv()

    def wait_sent(src, sem):
        wait_remote(src, sem).wait_send()

    small = [pltpu.make_async_copy(src, dst, small_sem.at[i])
             for i, (src, dst) in enumerate(((len_hbm, len_ref), (freq_hbm, freq_ref), (gain_hbm, gain_ref)))]
    for cp in small:
        cp.start()
    offs = [half]
    for d in range(half - 1, 0, -1):
        offs += [d, chips - d]
    offs += [0]
    for k in range(nch):
        x_copy(k).start()
    for k in range(FIRST):
        start_w(0, k, w_sem.at[k, 0], w_sem.at[k, 1])

    scope_pre = jax.named_scope("pre")
    scope_pre.__enter__()
    barrier = pltpu.get_barrier_semaphore()
    for d in range(1, tp):
        pl.semaphore_signal(barrier, inc=1, device_id={"tp": lax.rem(me + d, tp)}, device_id_type=pl.DeviceIdType.MESH)

    pad = wod.shape[1] - cw - ff
    if pad:
        for j in range(chips):
            wod[j, cw + ff:, :] = jnp.zeros((pad, 2 * cw), BF16)
        ut[ff:, :] = jnp.zeros((pad, rows), F32)
    for cp in small:
        cp.wait()
    for k in range(FIRST, AHEAD):
        start_w(0, k, w_sem.at[k, 0], w_sem.at[k, 1])
    gain_s[...] = gain_ref[...].astype(F32)
    lenb[...] = jnp.broadcast_to(len_ref[...].astype(F32), (rows, rows)).T
    scope_pre.__exit__(None, None, None)

    def set_inv_rms(ssq):
        inv = lax.rsqrt(ssq / width + NORM_EPS)
        rb[...] = jnp.broadcast_to(inv, rb.shape)

    def do_chunks(l, ks):
        nt = (((1,), (1,)), ((), ()))

        def join(parts, axis):
            return parts[0] if len(parts) == 1 else jnp.concatenate(parts, axis=axis)

        a = []
        for k in ks:
            g = gain_s[l:l + 1, pl.ds(pl.multiple_of(k * cw, cw), cw)]
            a.append((xg[l, k].astype(F32) * rb[...] * g).astype(BF16))
        a = join(a, 1)
        acc_qkv[...] += jnp.dot(a, join([wqkv[k] for k in ks], 0), preferred_element_type=F32)
        acc_g[...] += lax.dot_general(join([wgu[k, 0] for k in ks], 1), a, nt, preferred_element_type=F32)
        acc_u[...] += lax.dot_general(join([wgu[k, 1] for k in ks], 1), a, nt, preferred_element_type=F32)

    def rope(v):
        return (v * cosb[...] + pltpu.roll(v, head // 2, 1) * sinb[...]).astype(BF16).astype(F32)

    def zero_acc():
        acc_qkv[...] = jnp.zeros_like(acc_qkv)
        acc_g[...] = jnp.zeros_like(acc_g)
        acc_u[...] = jnp.zeros_like(acc_u)

    def attention(l):
        for h in range(hq):
            q = acc_qkv[:, h * head:(h + 1) * head].astype(BF16).astype(F32)
            k = acc_qkv[:, cw + h * head:cw + (h + 1) * head].astype(BF16).astype(F32)
            v = acc_qkv[:, 2 * cw + h * head:2 * cw + (h + 1) * head].astype(BF16).astype(F32)
            qs[:, h] = rope(q).reshape(ngrp, grp, head)
            ks[:, h] = rope(k).reshape(ngrp, grp, head)
            vs[:, h] = v.reshape(ngrp, grp, head)
        with jax.named_scope(f"kvwait{l}"):
            arrive(kbuf, kv_sem.at[0])
            arrive(vbuf, kv_sem.at[1])
        m = hq * grp
        for g in range(ngrp):
            q = qs[g].reshape(m, head).astype(BF16)
            kk = kbuf[g * gcols:(g + 1) * gcols, :]
            logit_s[g * m:(g + 1) * m, :] = lax.dot_general(q, kk, (((1,), (1,)), ((), ())), preferred_element_type=F32)
        col = lax.broadcasted_iota(jnp.int32, (m, gcols), 1)
        row = lax.broadcasted_iota(jnp.int32, (m, gcols), 0)
        same = ((col // (seq * hq)) == lax.rem(row, grp)) & (lax.rem(col, hq) == row // grp)
        key = jnp.where(same, lax.rem(col // hq, seq), 2 * seq).astype(F32)
        for g in range(ngrp):
            ln = lenb[g * grp:(g + 1) * grp, 0:1]
            ln = jnp.concatenate([ln] * hq, axis=0)
            lg = jnp.where(key < ln, logit_s[g * m:(g + 1) * m, :] * scale, -jnp.inf)
            qv = qs[g].reshape(m, head)
            kv = ks[g].reshape(m, head)
            vv = vs[g].reshape(m, head)
            sl = jnp.sum(qv * kv, axis=1, keepdims=True) * scale
            peak = jnp.maximum(jnp.max(lg, axis=1, keepdims=True), sl)
            w = jnp.exp(lg - peak)
            sw = jnp.exp(sl - peak)
            den = jnp.sum(w, axis=1, keepdims=True) + sw
            prob_s[g * m:(g + 1) * m, :] = (w / den).astype(BF16)
            sp = (sw / den).astype(BF16).astype(F32)
            vs[g] = (sp * vv).reshape(hq, grp, head)
        for g in range(ngrp):
            p = prob_s[g * m:(g + 1) * m, :]
            o = jnp.dot(p, vbuf[g * gcols:(g + 1) * gcols, :], preferred_element_type=F32)
            o = o + vs[g].reshape(m, head)
            for h in range(hq):
                attn_s[g * grp:(g + 1) * grp, h * head:(h + 1) * head] = o[h * grp:(h + 1) * grp]
        hbuf[:, 0:cw] = attn_s[...].astype(BF16)

    def mlp_act():
        gt = acc_g[...].astype(BF16).astype(F32)
        up = acc_u[...].astype(BF16).astype(F32)
        ut[0:ff, :] = gt * (1.0 / (1.0 + jnp.exp(-gt))) * up
        for i in range(ut.shape[0] // 128):
            hbuf[:, cw + i * 128:cw + (i + 1) * 128] = ut[i * 128:(i + 1) * 128, :].T.astype(BF16)

    def send_share(l, i, p):
        r = pl.ds(p * pr, pr)
        send(shr_snd.at[l, i, r, :], shr_rcv.at[l, i, r, :], rs_s_sem, rs_r_sem.at[p, i], ring_dev(offs[i]))

    def out_proj(l):
        hv = hbuf[...]

        def finish(i):
            off = offs[i]
            wait_recv(rcv_f.at[l, i], pair_r_sem.at[i])
            s = own_f[l, i] + rcv_f[l, i]
            if off == 0:
                own_f[l, i] = s
            else:
                shr_snd[l, i] = s.astype(BF16)
                send_share(l, i, 0)

        for i in range(chips):
            j = lax.rem(z + offs[i], chips)
            arrive(wod.at[j, 0:cw + ff, :], od_sem.at[i])
            p = jnp.dot(hv, wod[j], preferred_element_type=F32)
            lo, hi = p[:, :cw], p[:, cw:]
            own_f[l, i] = jnp.where(c == 0, lo, hi)
            snd_f[l, i] = jnp.where(c == 0, hi, lo)
            send(snd_f.at[l, i], rcv_f.at[l, i], pair_s_sem, pair_r_sem.at[i], partner)
            if i >= LAG:
                finish(i - LAG)
        for i in range(chips - LAG, chips):
            finish(i)
        for p in range(1, NSUB):
            for i in range(chips - 1):
                send_share(l, i, p)
        wait_sent(snd_f.at[l], pair_s_sem)

    def reduce_own(l, p):
        r = pl.ds(p * pr, pr)
        acc = xg[l, me, r, :].astype(F32) + own_f[l, chips - 1, r, :]
        for i in range(chips - 1):
            wait_recv(shr_rcv.at[l, i, r, :], rs_r_sem.at[p, i])
            acc = acc + shr_rcv[l, i, r, :].astype(F32)
        xg[l + 1, me, r, :] = acc.astype(BF16)

    def gather(l, use):
        dst = l + 1
        flip = 1 - 2 * c

        def piece(src, p):
            return xg.at[dst, src, pl.ds(p * pr, pr), :]

        def whole(src):
            return xg.at[dst, src]

        def slot(d, side):
            return 0 if d == 0 else (2 * half - 1 if d == half else 2 * d - 1 + side)

        def sem_of(d, side, p):
            return ag_r_sem.at[p * 2 + side] if d == 2 else ag_r_sem.at[2 * NSUB + (0 if d == half else (d // 2 + 1) * 2 - 1 + side)]

        def to_partner(ref, d, side):
            send(ref, ref, ag_s_sem, pf_r_sem.at[slot(d, side)], partner)

        def ring(ref, d, p, hops):
            send(ref, ref, ag_s_sem, sem_of(d, 0 if hops > 0 else 1, p), ring_dev(hops))

        def arrived(d, side):
            src = ring_dev(-d if side == 0 else d)
            wait_recv(whole(src), sem_of(d, side, 0))
            to_partner(whole(src), d, side)
            return src

        def from_partner(d, side):
            src = me + flip if d == 0 else ring_dev(-d if side == 0 else d) + flip
            wait_recv(whole(src), pf_r_sem.at[slot(d, side)])
            return src

        for p in range(NSUB):
            with jax.named_scope(f"reduce{l}p{p}"):
                reduce_own(l, p)
            ring(piece(me, p), 2, p, 2)
            ring(piece(me, p), 2, p, -2)
            if p == NSUB - 1:
                use("early", [])
            ring(piece(me, p), 1, p, 1)
            ring(piece(me, p), 1, p, -1)
            to_partner(piece(me, p), 0, 0)
        wait_sent(shr_snd.at[l, 0:chips - 1], rs_s_sem)
        use("own", [me])
        two = [ring_dev(-2), ring_dev(2)]
        for p in range(NSUB):
            for side in (0, 1):
                src = two[side]
                wait_recv(piece(src, p), sem_of(2, side, p))
                sg = 1 if side == 0 else -1
                if side == p // (NSUB // 2):
                    ring(piece(src, p), 4, p, 2 * sg)
                ring(piece(src, p), 3, p, sg)
                to_partner(piece(src, p), 2, side)
        one = [arrived(1, 0), arrived(1, 1)]
        use("ring", two + one)
        use("pair", [from_partner(0, 0), from_partner(2, 0), from_partner(2, 1)])
        three = [arrived(3, 0), arrived(3, 1)]
        far = [arrived(4, 0)]
        use("pair", [from_partner(1, 0), from_partner(1, 1)])
        use("ring", three + far)
        use("pair", [from_partner(3, 0), from_partner(3, 1)])
        use("pair", [from_partner(4, 0)])
        wait_sent(xg.at[dst, 0:7 + 2 * half], ag_s_sem)

    with jax.named_scope("stats"):
        ssq = jnp.zeros((rows, cw), F32)
        arrive(xg.at[0], x_sem)
        for k in range(nch):
            xf = xg[0, k].astype(F32)
            ssq = ssq + xf * xf
        set_inv_rms(jnp.sum(ssq, axis=1, keepdims=True))
        zero_acc()

    rope_rows = rows * UNROLL // nch

    def l0_body(i, carry):
        ks = [i * UNROLL + u for u in range(UNROLL)]
        for k in ks:
            b = lax.rem(k, RING)
            arrive(wqkv.at[k], w_sem.at[b, 0])
            arrive(wgu.at[k], w_sem.at[b, 1])
        for k in ks:
            @pl.when(k + AHEAD < nch)
            def _(k=k):
                nb = lax.rem(k + AHEAD, RING)
                start_w(0, k + AHEAD, w_sem.at[nb, 0], w_sem.at[nb, 1])

        @pl.when(i == KV_AT)
        def _():
            start_kv(0)
        for b in range(2):
            @pl.when(i == nch // UNROLL - 2 + b)
            def _(b=b):
                start_od(0, 2 * b)
                start_od(0, 2 * b + 1)
        r = pl.ds(pl.multiple_of(i * rope_rows, rope_rows), rope_rows)
        ang = lenb[r, :] * freq_ref[...]
        sn = jnp.sin(ang)
        cosb[r, :] = jnp.cos(ang)
        sinb[r, :] = jnp.where(lax.broadcasted_iota(jnp.int32, sn.shape, 1) < head // 2, -sn, sn)
        do_chunks(0, ks)
        return carry

    with jax.named_scope("kloop"):
        lax.fori_loop(0, nch // UNROLL, l0_body, 0)
        for b in range(4, chips):
            start_od(0, b)

    for l in range(layers):
        attention(l)
        with jax.named_scope(f"act{l}"):
            mlp_act()
        if l == 0:
            with jax.named_scope("barrier"):
                pl.semaphore_wait(barrier, tp - 1)
        with jax.named_scope(f"outproj{l}"):
            out_proj(l)
        if l + 1 < layers:
            for k in range(nch):
                start_w(l + 1, k, wl_sem.at[0], wl_sem.at[1])
            start_kv(l + 1)
            for i in range(chips):
                start_od(l + 1, i)
        if l + 1 < layers:
            def use(kind, srcs, l=l):
                if kind == "early":
                    xf = xg[l + 1, me].astype(F32)
                    sq = jnp.sum(xf * xf, axis=1, keepdims=True)
                    stats[l, me] = jnp.broadcast_to(sq, (rows, rows)).T[0:1, :]
                    for d in range(1, tp):
                        send(stats.at[l, me], stats.at[l, me], st_s_sem, st_r_sem, lax.rem(me + d, tp))
                    return
                if kind == "own":
                    zero_acc()
                    return
                if kind == "ring" and not use.ready:
                    use.ready = True
                    wait_recv(stats.at[l, 0:tp - 1], st_r_sem)
                    wait_sent(stats.at[l, 0:tp - 1], st_s_sem)
                    arrive(wqkv, wl_sem.at[0])
                    arrive(wgu, wl_sem.at[1])
                    tot = stats[l, 0]
                    for d in range(1, tp):
                        tot = tot + stats[l, d]
                    set_inv_rms(jnp.broadcast_to(tot, (rows, rows)).T[:, 0:1])
                    srcs = [me] + srcs
                for n in range(0, len(srcs), WIDE):
                    do_chunks(l + 1, srcs[n:n + WIDE])

            use.ready = False
            with jax.named_scope(f"gather{l}"):
                gather(l, use)
        else:
            def use_out(kind, srcs, l=l):
                for src in srcs:
                    out_ref[:, pl.ds(pl.multiple_of(src * cw, cw), cw)] = xg[l + 1, src]

            with jax.named_scope(f"gather{l}"):
                gather(l, use_out)


def solution(mesh):
    tp = mesh.shape["tp"]
    arg_specs = (P("dp", None), P("dp"), P(), P(None, None, "tp"), P(None, None, "tp"), P(None, None, "tp"), P(None, "tp", None),
                 P(None, None, "tp"), P(None, None, "tp"), P(None, "tp", None), P(None, "dp", None, "tp", None), P(None, "dp", None, "tp", None))

    def per_device(x_in, lengths, norm_gain, w_q, w_k, w_v, w_o, w_gate, w_up, w_down, k_cache, v_cache):
        rows, width = x_in.shape
        layers, _, seq, hq, head = k_cache.shape
        ff = w_gate.shape[2]
        cw = width // tp
        chips = tp // 2
        assert w_q.shape[2] == cw == hq * head
        freq = (1.0 / (np.float32(ROPE_BASE) ** (np.arange(0, head, 2).astype(np.float32) / np.float32(head)))).astype(np.float32)
        freq = jnp.asarray(np.concatenate([freq, freq])[None, :])
        ffp = -(-(cw + ff) // 256) * 256 - cw
        kvr = rows * seq * hq
        ngrp = rows // 8
        m = hq * 8
        pin = lambda v: pltpu.with_memory_space_constraint(v, pltpu.HBM)
        hbm = pl.BlockSpec(memory_space=pltpu.HBM)
        any_spec = pl.BlockSpec(memory_space=pl.ANY)
        vmem = pl.BlockSpec(memory_space=pltpu.VMEM)
        V = pltpu.VMEM
        D = pltpu.SemaphoreType.DMA
        scratch = [
            V((1, rows), jnp.int32), V((1, head), F32), V((layers, width), BF16),
            V((layers + 1, tp, rows, cw), BF16),
            V((tp, cw, 3 * cw), BF16),
            V((tp, 2, ff, cw), BF16),
            V((chips, cw + ffp, 2 * cw), BF16),
            V((kvr, head), BF16), V((kvr, head), BF16),
            V((layers, width), F32),
            V((rows, cw), F32),
            V((rows, rows), F32),
            V((rows, head), F32), V((rows, head), F32),
            V((rows, 3 * cw), F32),
            V((ff, rows), F32), V((ff, rows), F32),
            V((ffp, rows), F32),
            V((ngrp, hq, 8, head), F32), V((ngrp, hq, 8, head), F32), V((ngrp, hq, 8, head), F32),
            V((rows * hq, 8 * seq * hq), F32),
            V((rows * hq, 8 * seq * hq), BF16),
            V((rows, cw + ffp), BF16),
            V((rows, cw), F32),
            V((layers, chips, rows, cw), F32),
            V((layers, chips, rows, cw), F32),
            V((layers, chips, rows, cw), F32),
            V((layers, chips, rows, cw), BF16),
            V((layers, chips, rows, cw), BF16),
            V((layers, tp, 1, rows), F32),
            D((3,)), D(()), D((RING, 2)), D((2,)), D((2,)), D((chips,)),
            D(()), D((chips,)), D(()), D((NSUB, chips - 1)), D(()), D(()),
            D(()), D((2 * NSUB + 5,)), D((chips,)),
        ]
        cfg = (tp, rows, width, ff, seq, head, hq, layers)
        return pl.pallas_call(
            functools.partial(decode_kernel, cfg),
            out_shape=jax.ShapeDtypeStruct((rows, width), BF16),
            in_specs=[any_spec, hbm, hbm, hbm] + [any_spec] * 9,
            out_specs=vmem,
            scratch_shapes=scratch,
            compiler_params=pltpu.CompilerParams(collective_id=0, has_side_effects=True, vmem_limit_bytes=VLIM * 1024),
        )(x_in, pin(lengths.reshape(1, rows)), pin(freq), pin(norm_gain), w_q, w_k, w_v, w_o, jnp.swapaxes(w_gate, 1, 2), jnp.swapaxes(w_up, 1, 2), w_down,
          k_cache.reshape(layers, kvr, head), v_cache.reshape(layers, kvr, head))

    return jax.shard_map(per_device, mesh=mesh, in_specs=arg_specs, out_specs=P("dp", None), check_vma=False)
```
